32 devices in a mesh: scan: 2 (over y), chan: 4 (over z), tm: 2 (over x), pol: 2 (over core).
Axes of the slice: x: 2, y: 2, z: 4, core: 2. Of those that a mesh axis runs over, the one named last changes fastest.
Arguments:
- samples: int32 [2, 8, 4, 2, 16, 32768], P('pol', ('scan', 'tm'), None, None, None, 'chan'), parts along dimension 1, may hold values from 0 to 3
- pcal_phase: float32 [2, 16, 128], P('pol'), may hold values from -3.140625 to 3.140625
- tone_index: int32 [32768], P('chan'), may hold values from 0 to 127
- baseline_pairs: int32 [120, 2], replicated, may hold values from 0 to 15, as said below
Outputs:
- fringe_power: float32 [2, 8, 120, 8192], P('pol', ('scan', 'chan'), 'tm'), parts along dimension 1
The draws below stay inside these ranges and needn't reach their ends.
There are 2 independent parts, one for each index of `scan`. The reference program is written for one: setup_inputs(seed, part) draws one part's arguments, and reference() takes and returns one part's arrays. A program takes and returns all parts, laid end to end along the dimension named above; an argument that names none is the same for every part. Nothing has to cross between parts.
Inputs may be any that keep to these rules, and one draw needn't show every extreme that they name: `baseline_pairs`: each row holds two different stations; every unordered pair of the 16 stations stands in exactly one row, in either order.
All inputs are finite; a program needn't handle non-finite values.
Results may differ from the reference program's by a relative error of at most 0.0029.
Values may be sent and summed in bfloat16 or wider, within the bound.
A program may use at most 256 MiB of HBM per device.

```python
import jax
import jax.numpy as jnp
import numpy as np
from jax import lax

S = 16
NC = 32768
NTONE = 128
M = 4
NPOL = 2
NT = 4
ND = 8192


def draw_baseline_pairs(key, part):
    pair_table = np.array([(low_station, high_station) for low_station in range(S) for high_station in range(low_station + 1, S)], dtype=np.int32)
    pair_order = jax.random.permutation(key, pair_table.shape[0])
    picked_rows = jnp.asarray(pair_table)[pair_order]
    flipped = jax.random.randint(jax.random.fold_in(key, 7), (pair_table.shape[0],), 0, 2)
    first_station = jnp.where(flipped == 1, picked_rows[:, 1], picked_rows[:, 0])
    second_station = jnp.where(flipped == 1, picked_rows[:, 0], picked_rows[:, 1])
    return jnp.stack([first_station, second_station], axis=1).astype(jnp.int32)


def with_ends(result, stream_key, smallest, high):
    longest = result.shape.index(max(result.shape))
    spots = []
    for shift in (0, 1):
        where = [jax.random.randint(jax.random.fold_in(stream_key, axis), (), 0, length) for axis, length in enumerate(result.shape)]
        where[longest] = (where[longest] + shift) % result.shape[longest]
        spots.append(tuple(where))
    return result.at[spots[0]].set(smallest).at[spots[1]].set(high)


def setup_inputs(seed: int = 0, part: int = 0) -> dict:
    seeds = jax.random.split(jax.random.key(seed), 5)
    part_splits = jax.random.split(jax.random.fold_in(seeds[4], part), 5)
    return {
        "samples": with_ends(jax.random.randint(part_splits[0], (NPOL, NT, M, 2, S, NC), 0, 4), jax.random.fold_in(part_splits[0], 1), 0, 3).astype(jnp.int32),
        "pcal_phase": jnp.clip(jax.random.uniform(seeds[1], (NPOL, S, NTONE), jnp.float32, -3.140625, 3.140625), -3.140625, 3.140625),
        "tone_index": with_ends(jax.random.randint(seeds[2], (NC,), 0, NTONE), jax.random.fold_in(seeds[2], 1), 0, NTONE - 1).astype(jnp.int32),
        "baseline_pairs": draw_baseline_pairs(jax.random.fold_in(seeds[4], 71), part),
    }


def calibrated_period(block, first_index, second_index, cos_diff, sin_diff):
    levels = (2 * block - 3).astype(jnp.float32)
    first_volts = levels[:, :, first_index, :]
    second_volts = levels[:, :, second_index, :]
    raw_real = jnp.sum(first_volts[:, 0] * second_volts[:, 0] + first_volts[:, 1] * second_volts[:, 1], axis=0)
    raw_imag = jnp.sum(first_volts[:, 1] * second_volts[:, 0] - first_volts[:, 0] * second_volts[:, 1], axis=0)
    vis_real = raw_real * cos_diff + raw_imag * sin_diff
    vis_imag = raw_imag * cos_diff - raw_real * sin_diff
    return jnp.stack([vis_real, vis_imag], axis=1).astype(jnp.bfloat16)


def one_polarization(samples_pol, phase_pol, tone_index, baseline_pairs):
    first_index = baseline_pairs[:, 0]
    second_index = baseline_pairs[:, 1]
    cos_table = jnp.cos(phase_pol)[:, tone_index]
    sin_table = jnp.sin(phase_pol)[:, tone_index]
    cos_first = cos_table[first_index]
    sin_first = sin_table[first_index]
    cos_second = cos_table[second_index]
    sin_second = sin_table[second_index]
    cos_diff = cos_first * cos_second + sin_first * sin_second
    sin_diff = sin_first * cos_second - cos_first * sin_second

    def per_period(block):
        return calibrated_period(block, first_index, second_index, cos_diff, sin_diff)

    visibility = lax.map(per_period, samples_pol)
    values = visibility.astype(jnp.float32)
    spectra = jnp.fft.fft(lax.complex(values[:, :, 0], values[:, :, 1]), axis=0)
    lag_index = (jnp.arange(ND, dtype=jnp.int32) - ND // 2) % NC
    scale = 1.0 / (100.0 * M * NT * NC)

    def per_rate(rate_row):
        delays = jnp.fft.fft(rate_row, axis=-1)[:, lag_index]
        return (jnp.real(delays) * jnp.real(delays) + jnp.imag(delays) * jnp.imag(delays)) * scale

    return lax.map(per_rate, spectra)


def reference(samples, pcal_phase, tone_index, baseline_pairs):
    outputs = [one_polarization(samples[pol_index], pcal_phase[pol_index], tone_index, baseline_pairs) for pol_index in range(NPOL)]
    return jnp.stack(outputs, axis=0).astype(jnp.float32)
```

```python
import functools
import math

import jax
import jax.numpy as jnp
import numpy as np
from jax import lax
from jax.experimental import pallas as pl
from jax.experimental.pallas import tpu as pltpu
from jax.sharding import PartitionSpec as P

S = 16
NTONE = 128
ND = 8192
INNER = 256
GROUP = 3

highest = lax.Precision.HIGHEST
two_pi = 2.0 * math.pi
f32, bf16 = jnp.float32, jnp.bfloat16
MESH = pl.DeviceIdType.MESH


def split_hi_lo(value):
    high = np.asarray(value, np.float32).astype(bf16)
    low = (np.asarray(value, np.float64) - high.astype(np.float64)).astype(np.float32).astype(bf16)
    return high, low


def phase_table(left, right, modulus):
    angles = two_pi * (np.outer(left, right) % modulus) / modulus
    return np.cos(angles), np.sin(angles)


def tables(n_chan, depth):
    channels = n_chan * depth * INNER
    outer = channels // INNER
    wide = ND // outer
    outer_axis = np.arange(outer)
    inner_axis = np.arange(INNER)
    firsts = []
    for z in range(n_chan):
        fc, fs = phase_table(outer_axis, z * depth + np.arange(depth), outer)
        both = np.concatenate(
            [np.concatenate([fc, fs], axis=1), np.concatenate([-fs, fc], axis=1)], axis=0
        )
        firsts.append(np.concatenate(split_hi_lo(both), axis=1))
    twist_cos, twist_sin = phase_table(outer_axis, inner_axis, channels)
    lc, ls = phase_table(inner_axis, np.arange(wide) - wide // 2, INNER)
    last = np.concatenate(
        [np.concatenate([lc, -ls], axis=1), np.concatenate([ls, lc], axis=1)], axis=0
    )
    last = np.concatenate(split_hi_lo(last), axis=1)
    return np.stack(firsts), twist_cos.astype(np.float32), twist_sin.astype(np.float32), last


def add_scaled(total, value, factor):
    if abs(factor) < 1e-9:
        return total
    if abs(factor - 1.0) < 1e-9:
        return value if total is None else total + value
    if abs(factor + 1.0) < 1e-9:
        return -value if total is None else total - value
    return value * factor if total is None else total + value * factor


def flip_bits(z, q):
    out, bit = z, 1
    while bit <= q:
        if q & bit:
            out = out + bit * (1 - 2 * lax.rem(lax.div(z, bit), 2))
        bit *= 2
    return out


def kernel(n_tm, n_chan, group, scale, *refs):
    steps = n_chan.bit_length() - 1
    (pairs, x_ref, cos_ref, sin_ref, first_ref, tcos_ref, tsin_ref, last_ref), refs = refs[:8], refs[8:]
    out_ref, vis, outbox, twisted, spec, keep = refs[:6]
    sends, recvs = refs[6 : 6 + steps], refs[6 + steps : 6 + 2 * steps]
    tm_send, tm_recv, ch_send, ch_recv = refs[6 + 2 * steps :]

    periods, samples, _, _, depth, inner = x_ref.shape
    count = vis.shape[1]
    chunks = count // group
    rates = periods * n_tm
    outer = tcos_ref.shape[0]
    lanes = last_ref.shape[1] // 2
    me = lax.axis_index("tm")
    z = lax.axis_index("chan")

    barrier = pltpu.get_barrier_semaphore()
    for slot in range(1, n_tm):
        pl.semaphore_signal(
            barrier, inc=1, device_id={"tm": lax.rem(me + slot, n_tm)}, device_id_type=MESH
        )
    for step in range(steps):
        pl.semaphore_signal(
            barrier, inc=1, device_id={"chan": flip_bits(z, 1 << step)}, device_id_type=MESH
        )
    pl.semaphore_wait(barrier, n_tm - 1 + steps)

    def rows(chunk):
        return pl.ds(chunk * group, group)

    def tm_copy(slot, chunk):
        return pltpu.make_async_remote_copy(
            src_ref=outbox.at[slot - 1, rows(chunk)],
            dst_ref=vis.at[slot, rows(chunk)],
            send_sem=tm_send.at[slot - 1, chunk],
            recv_sem=tm_recv.at[slot - 1, chunk],
            device_id={"tm": lax.rem(me + slot, n_tm)},
            device_id_type=MESH,
        )

    def chan_copy(step, chunk):
        return pltpu.make_async_remote_copy(
            src_ref=sends[step].at[rows(chunk)],
            dst_ref=recvs[step].at[rows(chunk)],
            send_sem=ch_send.at[step, chunk],
            recv_sem=ch_recv.at[step, chunk],
            device_id={"chan": flip_bits(z, 1 << step)},
            device_id_type=MESH,
        )

    def correlate(slot, chunk):
        base = lax.rem(me + slot, n_tm) * count
        target, index = (vis, 0) if slot == 0 else (outbox, slot - 1)

        def one(k, carry):
            row = chunk * group + k
            a = pairs[base + row, 0]
            e = pairs[base + row, 1]
            ca, sa = cos_ref[a], sin_ref[a]
            ce, se = cos_ref[e], sin_ref[e]
            cos_diff = ca * ce + sa * se
            sin_diff = sa * ce - ca * se
            for period in range(periods):
                real = imag = None
                for m in range(samples):
                    ar, ai = x_ref[period, m, 0, a], x_ref[period, m, 1, a]
                    er, ei = x_ref[period, m, 0, e], x_ref[period, m, 1, e]
                    step_real = ar * er + ai * ei
                    step_imag = ai * er - ar * ei
                    real = step_real if real is None else real + step_real
                    imag = step_imag if imag is None else imag + step_imag
                real, imag = real.astype(f32), imag.astype(f32)
                both = jnp.concatenate(
                    [real * cos_diff + imag * sin_diff, imag * cos_diff - real * sin_diff], axis=0
                )
                target[index, row, period] = both.astype(bf16)
            return carry

        lax.fori_loop(0, group, one, 0)

    def outgoing(chunk):
        for slot in range(1, n_tm):
            correlate(slot, chunk)
            tm_copy(slot, chunk).start()

    def delay(chunk):
        for slot in range(1, n_tm):
            tm_copy(slot, chunk).wait_recv()

        def one(k, carry):
            row = chunk * group + k
            for slot in range(n_tm):
                for period in range(periods):
                    value = vis[slot, row, period]
                    section = jnp.dot(
                        first_ref[...],
                        jnp.concatenate([value, value], axis=0),
                        preferred_element_type=f32,
                    )
                    yr, yi = section[:outer], section[outer:]
                    tr = yr * tcos_ref[...] + yi * tsin_ref[...]
                    ti = yi * tcos_ref[...] - yr * tsin_ref[...]
                    place = slot * periods + period
                    twisted[place * outer : (place + 1) * outer, :inner] = tr.astype(bf16)
                    twisted[place * outer : (place + 1) * outer, inner:] = ti.astype(bf16)
            parts = []
            sign = jnp.where(
                lax.broadcasted_iota(jnp.int32, (outer, lanes), 1) < lanes // 2, 1.0, -1.0
            )
            for slot in range(n_tm):
                for period in range(periods):
                    place = slot * periods + period
                    both = jnp.dot(
                        twisted[place * outer : (place + 1) * outer],
                        last_ref[...],
                        preferred_element_type=f32,
                    )
                    value = both[:, :lanes] + both[:, lanes:]
                    turned = pltpu.roll(value, lanes // 2, 1) * sign
                    parts.append(((period - periods * slot) % rates, value, turned))
            for rate in range(rates):
                total = None
                for when, value, turned in parts:
                    angle = two_pi * (rate * when % rates) / rates
                    total = add_scaled(total, value, math.cos(angle))
                    total = add_scaled(total, turned, math.sin(angle))
                spec[rate] = total
            for q in range(rates):
                value = spec[flip_bits(z, q)]
                if q % 2 == 0:
                    keep[row, q // 2] = value
                else:
                    sends[0][row, q // 2] = value.astype(bf16)
            return carry

        lax.fori_loop(0, group, one, 0)
        chan_copy(0, chunk).start()

    def combine(step, chunk):
        chan_copy(step, chunk).wait_recv()

        def one(k, carry):
            row = chunk * group + k
            for j in range(recvs[step].shape[1]):
                total = keep[row, j << step] + recvs[step][row, j].astype(f32)
                if step == steps - 1:
                    turned = jnp.transpose(total)
                    half = lanes // 2
                    out_ref[row] = (turned[:half] ** 2 + turned[half:] ** 2) * scale
                elif j % 2 == 0:
                    keep[row, j << step] = total
                else:
                    sends[step + 1][row, j // 2] = total.astype(bf16)
            return carry

        lax.fori_loop(0, group, one, 0)
        if step < steps - 1:
            chan_copy(step + 1, chunk).start()

    outgoing(0)

    def round_trip(i, carry):
        @pl.when(i + 1 < chunks)
        def _():
            outgoing(i + 1)

        @pl.when(i < chunks)
        def _():
            correlate(0, i)
            delay(i)

        for step in range(steps):
            lag = step + 1

            @pl.when((i >= lag) & (i - lag < chunks))
            def _():
                combine(step, i - lag)

        return carry

    lax.fori_loop(0, chunks + steps, round_trip, 0)

    def drain(i, carry):
        for slot in range(1, n_tm):
            tm_copy(slot, i).wait_send()
        for step in range(steps):
            chan_copy(step, i).wait_send()
        return carry

    lax.fori_loop(0, chunks, drain, 0)


def fringe(n_tm, n_chan, pairs, x, cosine, sine, first, twist_cos, twist_sin, last):
    steps = n_chan.bit_length() - 1
    periods, samples, _, _, depth, inner = x.shape
    rates = periods * n_tm
    count = pairs.shape[0] // n_tm
    group = max(g for g in range(1, GROUP + 1) if count % g == 0)
    chunks = count // group
    outer = twist_cos.shape[0]
    lanes = last.shape[1] // 2
    channels = n_chan * depth * inner
    scale = 1.0 / (100.0 * samples * rates * channels)
    tile = (outer, lanes)
    boxes = [pltpu.VMEM((count, rates >> (s + 1)) + tile, bf16) for s in range(steps)]
    vmem = pl.BlockSpec(memory_space=pltpu.VMEM)
    return pl.pallas_call(
        functools.partial(kernel, n_tm, n_chan, group, scale),
        out_shape=jax.ShapeDtypeStruct((count, lanes // 2, outer), f32),
        in_specs=[pl.BlockSpec(memory_space=pltpu.SMEM)] + [vmem] * 7,
        out_specs=vmem,
        scratch_shapes=[
            pltpu.VMEM((n_tm, count, periods, 2 * depth, inner), bf16),
            pltpu.VMEM((n_tm - 1, count, periods, 2 * depth, inner), bf16),
            pltpu.VMEM((rates * outer, 2 * inner), bf16),
            pltpu.VMEM((rates,) + tile, f32),
            pltpu.VMEM((count, rates // 2) + tile, f32),
        ]
        + boxes
        + boxes
        + [
            pltpu.SemaphoreType.DMA((n_tm - 1, chunks)),
            pltpu.SemaphoreType.DMA((n_tm - 1, chunks)),
            pltpu.SemaphoreType.DMA((steps, chunks)),
            pltpu.SemaphoreType.DMA((steps, chunks)),
        ],
        compiler_params=pltpu.CompilerParams(
            collective_id=0, has_side_effects=True, vmem_limit_bytes=60 << 20
        ),
        name="fringe",
    )(pairs, x, cosine, sine, first, twist_cos, twist_sin, last)


def shards(samples, pcal_phase, tone_index, baseline_pairs):
    n_tm = lax.axis_size("tm")
    n_chan = lax.axis_size("chan")
    z = lax.axis_index("chan")
    _, nt_dev, m, _, _, width = samples.shape
    depth = width // INNER

    x = (2 * samples[0] - 3).astype(bf16).reshape(nt_dev, m, 2, S, depth, INNER)
    tone_slots = (tone_index[None, :] == jnp.arange(NTONE, dtype=jnp.int32)[:, None]).astype(f32)
    cosine = jnp.dot(jnp.cos(pcal_phase[0]), tone_slots, precision=highest).reshape(S, depth, INNER)
    sine = jnp.dot(jnp.sin(pcal_phase[0]), tone_slots, precision=highest).reshape(S, depth, INNER)

    firsts, twist_cos, twist_sin, last = tables(n_chan, depth)
    first = lax.dynamic_index_in_dim(jnp.asarray(firsts), z, 0, keepdims=False)
    power = fringe(
        n_tm, n_chan, baseline_pairs, x, cosine, sine, first,
        jnp.asarray(twist_cos), jnp.asarray(twist_sin), jnp.asarray(last),
    )
    return power.reshape(1, 1, power.shape[0], ND)


def solution(mesh):
    placed = (
        P("pol", ("scan", "tm"), None, None, None, "chan"),
        P("pol", None, None),
        P("chan"),
        P(),
    )
    return jax.shard_map(
        shards,
        mesh=mesh,
        in_specs=placed,
        out_specs=P("pol", ("scan", "chan"), "tm", None),
        check_vma=False,
    )
```

```python
import functools
import math

import jax
import jax.numpy as jnp
import numpy as np
from jax import lax
from jax.experimental import pallas as pl
from jax.experimental.pallas import tpu as pltpu
from jax.sharding import PartitionSpec as P

S = 16
ND = 8192
LANES = 128
SUB = 8
INNER = 256
GROUP = 1
AHEAD = 2
LAG = 3

two_pi = 2.0 * math.pi
f32, bf16 = jnp.float32, jnp.bfloat16
MESH = pl.DeviceIdType.MESH


def split_hi_lo(value):
    high = np.asarray(value, np.float32).astype(bf16)
    low = (np.asarray(value, np.float64) - high.astype(np.float64)).astype(np.float32).astype(bf16)
    return high, low


def phase_table(left, right, modulus):
    angles = two_pi * (np.outer(left, right) % modulus) / modulus
    return np.cos(angles), np.sin(angles)


def tables(n_chan, depth):
    channels = n_chan * depth * INNER
    outer = channels // INNER
    wide = ND // outer
    outer_axis = np.arange(outer)
    inner_axis = np.arange(INNER)
    firsts = []
    for z in range(n_chan):
        fc, fs = phase_table(outer_axis, z * depth + np.arange(depth), outer)
        both = np.concatenate(
            [np.concatenate([fc, fs], axis=1), np.concatenate([-fs, fc], axis=1)], axis=0
        )
        firsts.append(np.concatenate(split_hi_lo(both), axis=1))
    twist_cos, twist_sin = phase_table(outer_axis, inner_axis, channels)
    lc, ls = phase_table(inner_axis, np.arange(wide) - wide // 2, INNER)
    last = np.concatenate(
        [np.concatenate([lc, -ls], axis=1), np.concatenate([ls, lc], axis=1)], axis=0
    )
    last = np.concatenate(split_hi_lo(last), axis=1)
    return np.stack(firsts), twist_cos.astype(np.float32), twist_sin.astype(np.float32), last


def add_scaled(total, value, factor):
    if abs(factor) < 1e-9:
        return total
    if abs(factor - 1.0) < 1e-9:
        return value if total is None else total + value
    if abs(factor + 1.0) < 1e-9:
        return -value if total is None else total - value
    return value * factor if total is None else total + value * factor


def flip_bits(z, q):
    out, bit = z, 1
    while bit <= q:
        if q & bit:
            out = out + bit * (1 - 2 * lax.rem(lax.div(z, bit), 2))
        bit *= 2
    return out


def kernel(n_tm, n_chan, group, scale, *refs):
    steps = n_chan.bit_length() - 1
    (pairs, samples_ref, tones_in, pcal_in, firsts, *tables_in), refs = refs[:8], refs[8:]
    (out_ref, codes, x_ref, tones, pcal, cos_ref, sin_ref), refs = refs[:7], refs[7:]
    (first_ref, tcos_ref, tsin_ref, last_ref), refs = refs[:4], refs[4:]
    (vis, outbox, twisted, spec, keep), refs = refs[:5], refs[5:]
    sends, recvs = refs[:steps], refs[steps : 2 * steps]
    phase_sem, code_sem, table_sem, tm_send, tm_recv, ch_send, ch_recv = refs[2 * steps :]

    periods, samples, _, stations, depth, inner = x_ref.shape
    count = vis.shape[1]
    chunks = count // group
    rates = periods * n_tm
    outer = tcos_ref.shape[0]
    lanes = last_ref.shape[1] // 2
    halves = inner // LANES
    me = lax.axis_index("tm")
    z = lax.axis_index("chan")

    phases = [
        pltpu.make_async_copy(tones_in, tones, phase_sem.at[0]),
        pltpu.make_async_copy(pcal_in.at[0], pcal, phase_sem.at[1]),
    ]
    fetches = [
        pltpu.make_async_copy(samples_ref.at[period], codes.at[period], code_sem.at[period])
        for period in range(periods)
    ]
    for copy in phases + fetches:
        copy.start()
    constants = [
        pltpu.make_async_copy(source, target, table_sem.at[i])
        for i, (source, target) in enumerate(
            zip([firsts.at[z]] + tables_in, [first_ref, tcos_ref, tsin_ref, last_ref])
        )
    ]
    for copy in constants:
        copy.start()

    barrier = pltpu.get_barrier_semaphore()
    for slot in range(1, n_tm):
        pl.semaphore_signal(
            barrier, inc=1, device_id={"tm": lax.rem(me + slot, n_tm)}, device_id_type=MESH
        )
    for step in range(steps):
        pl.semaphore_signal(
            barrier, inc=1, device_id={"chan": flip_bits(z, 1 << step)}, device_id_type=MESH
        )

    def station_table(station, carry):
        phase = pcal[pl.ds(station, 1), :]
        for turn, target in ((jnp.cos, cos_ref), (jnp.sin, sin_ref)):
            row = jnp.broadcast_to(turn(phase), (depth, LANES))
            for half in range(halves):
                index = tones[pl.ds(half, depth, stride=halves), :]
                target[station, :, half * LANES : (half + 1) * LANES] = jnp.take_along_axis(
                    row, index, axis=1
                )
        return carry

    for copy in phases:
        copy.wait()
    lax.fori_loop(0, stations, station_table, 0)

    for period in range(periods):
        fetches[period].wait()

        def levels(station, carry):
            for m in range(samples):
                for part in range(2):
                    for half in range(halves):
                        start = lax.div(station, SUB) * (depth * halves * SUB) + half * SUB
                        code = codes[
                            period,
                            m,
                            part,
                            pl.ds(start + lax.rem(station, SUB), depth, stride=halves * SUB),
                            :,
                        ]
                        x_ref[
                            period, m, part, station, :, half * LANES : (half + 1) * LANES
                        ] = (2 * code - 3).astype(f32).astype(bf16)
            return carry

        lax.fori_loop(0, stations, levels, 0)
    for copy in constants:
        copy.wait()
    pl.semaphore_wait(barrier, n_tm - 1 + steps)

    def rows(chunk):
        return pl.ds(chunk * group, group)

    everything = pl.ds(0, count)

    def tm_copy(slot, chunk, block=None):
        block = rows(chunk) if block is None else block
        return pltpu.make_async_remote_copy(
            src_ref=outbox.at[slot - 1, block],
            dst_ref=vis.at[slot, block],
            send_sem=tm_send.at[slot - 1],
            recv_sem=tm_recv.at[slot - 1, chunk],
            device_id={"tm": lax.rem(me + slot, n_tm)},
            device_id_type=MESH,
        )

    def chan_copy(step, chunk, block=None):
        block = rows(chunk) if block is None else block
        return pltpu.make_async_remote_copy(
            src_ref=sends[step].at[block],
            dst_ref=recvs[step].at[block],
            send_sem=ch_send.at[step],
            recv_sem=ch_recv.at[step, chunk],
            device_id={"chan": flip_bits(z, 1 << step)},
            device_id_type=MESH,
        )

    def correlate(slot, chunk):
        base = lax.rem(me + slot, n_tm) * count
        target, index = (vis, 0) if slot == 0 else (outbox, slot - 1)

        def one(k, carry):
            row = chunk * group + k
            a = pairs[0, base + row]
            e = pairs[1, base + row]
            ca, sa = cos_ref[a], sin_ref[a]
            ce, se = cos_ref[e], sin_ref[e]
            cos_diff = ca * ce + sa * se
            sin_diff = sa * ce - ca * se
            for period in range(periods):
                real = imag = None
                for m in range(samples):
                    ar, ai = x_ref[period, m, 0, a], x_ref[period, m, 1, a]
                    er, ei = x_ref[period, m, 0, e], x_ref[period, m, 1, e]
                    step_real = ar * er + ai * ei
                    step_imag = ai * er - ar * ei
                    real = step_real if real is None else real + step_real
                    imag = step_imag if imag is None else imag + step_imag
                real, imag = real.astype(f32), imag.astype(f32)
                both = jnp.concatenate(
                    [real * cos_diff + imag * sin_diff, imag * cos_diff - real * sin_diff], axis=0
                )
                target[index, row, period] = both.astype(bf16)
            return carry

        lax.fori_loop(0, group, one, 0)

    def outgoing(chunk):
        for slot in range(1, n_tm):
            correlate(slot, chunk)
            tm_copy(slot, chunk).start()

    def delay(chunk):
        for slot in range(1, n_tm):
            tm_copy(slot, chunk).wait_recv()

        def one(k, carry):
            row = chunk * group + k
            for slot in range(n_tm):
                for period in range(periods):
                    value = vis[slot, row, period]
                    section = jnp.dot(
                        first_ref[...],
                        jnp.concatenate([value, value], axis=0),
                        preferred_element_type=f32,
                    )
                    yr, yi = section[:outer], section[outer:]
                    tr = yr * tcos_ref[...] + yi * tsin_ref[...]
                    ti = yi * tcos_ref[...] - yr * tsin_ref[...]
                    place = slot * periods + period
                    twisted[place * outer : (place + 1) * outer, :inner] = tr.astype(bf16)
                    twisted[place * outer : (place + 1) * outer, inner:] = ti.astype(bf16)
            parts = []
            sign = jnp.where(
                lax.broadcasted_iota(jnp.int32, (outer, lanes), 1) < lanes // 2, 1.0, -1.0
            )
            for slot in range(n_tm):
                for period in range(periods):
                    place = slot * periods + period
                    both = jnp.dot(
                        twisted[place * outer : (place + 1) * outer],
                        last_ref[...],
                        preferred_element_type=f32,
                    )
                    value = both[:, :lanes] + both[:, lanes:]
                    turned = pltpu.roll(value, lanes // 2, 1) * sign
                    parts.append(((period - periods * slot) % rates, value, turned))
            for rate in range(rates):
                total = None
                for when, value, turned in parts:
                    angle = two_pi * (rate * when % rates) / rates
                    total = add_scaled(total, value, math.cos(angle))
                    total = add_scaled(total, turned, math.sin(angle))
                spec[rate] = total
            for q in range(rates):
                value = spec[flip_bits(z, q)]
                if q % 2 == 0:
                    keep[row, q // 2] = value
                else:
                    sends[0][row, q // 2] = value.astype(bf16)
            return carry

        lax.fori_loop(0, group, one, 0)
        chan_copy(0, chunk).start()

    def combine(step, chunk):
        chan_copy(step, chunk).wait_recv()

        def one(k, carry):
            row = chunk * group + k
            for j in range(recvs[step].shape[1]):
                total = keep[row, j << step] + recvs[step][row, j].astype(f32)
                if step == steps - 1:
                    turned = jnp.transpose(total)
                    half = lanes // 2
                    out_ref[row] = (turned[:half] ** 2 + turned[half:] ** 2) * scale
                elif j % 2 == 0:
                    keep[row, j << step] = total
                else:
                    sends[step + 1][row, j // 2] = total.astype(bf16)
            return carry

        lax.fori_loop(0, group, one, 0)
        if step < steps - 1:
            chan_copy(step + 1, chunk).start()

    for i in range(min(AHEAD, chunks)):
        outgoing(i)

    def round_trip(i, carry):
        @pl.when(i + AHEAD < chunks)
        def _():
            outgoing(i + AHEAD)

        @pl.when(i < chunks)
        def _():
            correlate(0, i)
            delay(i)

        for step in range(steps):
            lag = LAG * (step + 1)

            @pl.when((i >= lag) & (i - lag < chunks))
            def _():
                combine(step, i - lag)

        return carry

    lax.fori_loop(0, chunks + steps * LAG, round_trip, 0)

    for slot in range(1, n_tm):
        tm_copy(slot, 0, everything).wait_send()
    for step in range(steps):
        chan_copy(step, 0, everything).wait_send()


def fringe(n_tm, n_chan, pairs, tones, pcal_phase, samples):
    steps = n_chan.bit_length() - 1
    _, periods, taken, _, stations, width = samples.shape
    depth = width // INNER
    rowed = samples.reshape(periods, taken, 2, stations // SUB, SUB, width // LANES, LANES)
    rowed = rowed.transpose(0, 1, 2, 3, 5, 4, 6).reshape(periods, taken, 2, -1, LANES)
    rates = periods * n_tm
    count = pairs.shape[1] // n_tm
    group = max(g for g in range(1, GROUP + 1) if count % g == 0)
    chunks = count // group
    constants = tables(n_chan, depth)
    firsts, twist_cos, _, last = constants
    outer = twist_cos.shape[0]
    lanes = last.shape[1] // 2
    scale = 1.0 / (100.0 * taken * rates * n_chan * width)
    tile = (outer, lanes)
    boxes = [pltpu.VMEM((count, rates >> (s + 1)) + tile, bf16) for s in range(steps)]
    vmem = pl.BlockSpec(memory_space=pltpu.VMEM)
    stay = pl.BlockSpec(memory_space=pltpu.HBM)
    return pl.pallas_call(
        functools.partial(kernel, n_tm, n_chan, group, scale),
        out_shape=pltpu.VMEM((count, lanes // 2, outer), f32),
        in_specs=[pl.BlockSpec(memory_space=pltpu.SMEM)] + [stay] * 7,
        out_specs=vmem,
        scratch_shapes=[
            pltpu.VMEM((periods, taken, 2, width // LANES * stations, LANES), jnp.int32),
            pltpu.VMEM((periods, taken, 2, stations, depth, INNER), bf16),
            pltpu.VMEM(tones.shape, jnp.int32),
            pltpu.VMEM(pcal_phase.shape[1:], f32),
            pltpu.VMEM((stations, depth, INNER), f32),
            pltpu.VMEM((stations, depth, INNER), f32),
            pltpu.VMEM(firsts.shape[1:], bf16),
            pltpu.VMEM(twist_cos.shape, f32),
            pltpu.VMEM(twist_cos.shape, f32),
            pltpu.VMEM(last.shape, bf16),
            pltpu.VMEM((n_tm, count, periods, 2 * depth, INNER), bf16),
            pltpu.VMEM((n_tm - 1, count, periods, 2 * depth, INNER), bf16),
            pltpu.VMEM((rates * outer, 2 * INNER), bf16),
            pltpu.VMEM((rates,) + tile, f32),
            pltpu.VMEM((count, rates // 2) + tile, f32),
        ]
        + boxes
        + boxes
        + [
            pltpu.SemaphoreType.DMA((2,)),
            pltpu.SemaphoreType.DMA((periods,)),
            pltpu.SemaphoreType.DMA((len(constants),)),
            pltpu.SemaphoreType.DMA((n_tm - 1,)),
            pltpu.SemaphoreType.DMA((n_tm - 1, chunks)),
            pltpu.SemaphoreType.DMA((steps,)),
            pltpu.SemaphoreType.DMA((steps, chunks)),
        ],
        compiler_params=pltpu.CompilerParams(
            collective_id=0, has_side_effects=True, vmem_limit_bytes=57 << 20
        ),
        name="fringe",
    )(pairs, rowed, tones, pcal_phase, *(jnp.asarray(c) for c in constants))


def shards(samples, pcal_phase, tone_index, baseline_pairs):
    power = fringe(
        lax.axis_size("tm"),
        lax.axis_size("chan"),
        baseline_pairs.T,
        tone_index.reshape(-1, LANES),
        pcal_phase,
        samples,
    )
    return power.reshape(1, 1, power.shape[0], ND)


def solution(mesh):
    placed = (
        P("pol", ("scan", "tm"), None, None, None, "chan"),
        P("pol", None, None),
        P("chan"),
        P(),
    )
    return jax.shard_map(
        shards,
        mesh=mesh,
        in_specs=placed,
        out_specs=P("pol", ("scan", "chan"), "tm", None),
        check_vma=False,
    )
```

```python
import functools
import math

import jax
import jax.numpy as jnp
import numpy as np
from jax import lax
from jax.experimental import pallas as pl
from jax.experimental.pallas import tpu as pltpu
from jax.sharding import PartitionSpec as P

S = 16
ND = 8192
LANES = 128
SUB = 8
INNER = 256
GROUP = 1
AHEAD = 2
LAG = 3
LENT = 8
FAR_AHEAD = 16
LENT_AHEAD = 10

two_pi = 2.0 * math.pi
f32, bf16 = jnp.float32, jnp.bfloat16
MESH = pl.DeviceIdType.MESH


def split_hi_lo(value):
    high = np.asarray(value, np.float32).astype(bf16)
    low = (np.asarray(value, np.float64) - high.astype(np.float64)).astype(np.float32).astype(bf16)
    return high, low


def phase_table(left, right, modulus):
    angles = two_pi * (np.outer(left, right) % modulus) / modulus
    return np.cos(angles), np.sin(angles)


def tables(n_chan, depth):
    channels = n_chan * depth * INNER
    outer = channels // INNER
    wide = ND // outer
    outer_axis = np.arange(outer)
    inner_axis = np.arange(INNER)
    firsts = []
    for z in range(n_chan):
        fc, fs = phase_table(outer_axis, z * depth + np.arange(depth), outer)
        both = np.concatenate(
            [np.concatenate([fc, fs], axis=1), np.concatenate([-fs, fc], axis=1)], axis=0
        )
        firsts.append(np.concatenate(split_hi_lo(both), axis=1))
    twist_cos, twist_sin = phase_table(outer_axis, inner_axis, channels)
    lc, ls = phase_table(inner_axis, np.arange(wide) - wide // 2, INNER)
    last = np.concatenate(
        [np.concatenate([lc, -ls], axis=1), np.concatenate([ls, lc], axis=1)], axis=0
    )
    last = np.concatenate(split_hi_lo(last), axis=1)
    return np.stack(firsts), twist_cos.astype(np.float32), twist_sin.astype(np.float32), last


def add_scaled(total, value, factor):
    if abs(factor) < 1e-9:
        return total
    if abs(factor - 1.0) < 1e-9:
        return value if total is None else total + value
    if abs(factor + 1.0) < 1e-9:
        return -value if total is None else total - value
    return value * factor if total is None else total + value * factor


def flip_bits(z, q):
    out, bit = z, 1
    while bit <= q:
        if q & bit:
            out = out + bit * (1 - 2 * lax.rem(lax.div(z, bit), 2))
        bit *= 2
    return out


def kernel(n_tm, n_chan, group, scale, *refs):
    steps = n_chan.bit_length() - 1
    (pairs, samples_ref, tones_in, pcal_in, firsts, *tables_in), refs = refs[:8], refs[8:]
    (out_ref, codes, x_ref, tones, pcal, cos_ref, sin_ref), refs = refs[:7], refs[7:]
    (first_ref, tcos_ref, tsin_ref, last_ref), refs = refs[:4], refs[4:]
    (vis, outbox, twisted, spec, keep), refs = refs[:5], refs[5:]
    sends, recvs = refs[:steps], refs[steps : 2 * steps]
    phase_sem, code_sem, table_sem, tm_send, tm_recv, ch_send, ch_recv = refs[2 * steps :]

    periods, samples, _, stations, depth, inner = x_ref.shape
    count = vis.shape[1]
    chunks = count // group
    rates = periods * n_tm
    outer = tcos_ref.shape[0]
    lanes = last_ref.shape[1] // 2
    halves = inner // LANES
    me = lax.axis_index("tm")
    z = lax.axis_index("chan")

    phases = [
        pltpu.make_async_copy(tones_in, tones, phase_sem.at[0]),
        pltpu.make_async_copy(pcal_in.at[0], pcal, phase_sem.at[1]),
    ]
    fetches = [
        pltpu.make_async_copy(samples_ref.at[period], codes.at[period], code_sem.at[period])
        for period in range(periods)
    ]
    for copy in phases + fetches:
        copy.start()
    constants = [
        pltpu.make_async_copy(source, target, table_sem.at[i])
        for i, (source, target) in enumerate(
            zip([firsts.at[z]] + tables_in, [first_ref, tcos_ref, tsin_ref, last_ref])
        )
    ]
    for copy in constants:
        copy.start()

    barrier = pltpu.get_barrier_semaphore()
    for slot in range(1, n_tm):
        pl.semaphore_signal(
            barrier, inc=1, device_id={"tm": lax.rem(me + slot, n_tm)}, device_id_type=MESH
        )
    for step in range(steps):
        pl.semaphore_signal(
            barrier, inc=1, device_id={"chan": flip_bits(z, 1 << step)}, device_id_type=MESH
        )

    def station_table(station, carry):
        phase = pcal[pl.ds(station, 1), :]
        for turn, target in ((jnp.cos, cos_ref), (jnp.sin, sin_ref)):
            row = jnp.broadcast_to(turn(phase), (depth, LANES))
            for half in range(halves):
                index = tones[pl.ds(half, depth, stride=halves), :]
                target[station, :, half * LANES : (half + 1) * LANES] = jnp.take_along_axis(
                    row, index, axis=1
                )
        return carry

    for copy in phases:
        copy.wait()
    lax.fori_loop(0, stations, station_table, 0)

    for period in range(periods):
        fetches[period].wait()

        def levels(station, carry):
            for m in range(samples):
                for part in range(2):
                    for half in range(halves):
                        start = lax.div(station, SUB) * (depth * halves * SUB) + half * SUB
                        code = codes[
                            period,
                            m,
                            part,
                            pl.ds(start + lax.rem(station, SUB), depth, stride=halves * SUB),
                            :,
                        ]
                        x_ref[
                            period, m, part, station, :, half * LANES : (half + 1) * LANES
                        ] = (2 * code - 3).astype(f32).astype(bf16)
            return carry

        lax.fori_loop(0, stations, levels, 0)
    for copy in constants:
        copy.wait()
    pl.semaphore_wait(barrier, n_tm - 1 + steps)

    def rows(chunk):
        return pl.ds(chunk * group, group)

    everything = pl.ds(0, count)

    def tm_copy(slot, chunk, block=None):
        block = rows(chunk) if block is None else block
        return pltpu.make_async_remote_copy(
            src_ref=outbox.at[slot - 1, block],
            dst_ref=vis.at[slot, block],
            send_sem=tm_send.at[slot - 1],
            recv_sem=tm_recv.at[slot - 1, chunk],
            device_id={"tm": lax.rem(me + slot, n_tm)},
            device_id_type=MESH,
        )

    def chan_copy(step, chunk, block=None):
        block = rows(chunk) if block is None else block
        return pltpu.make_async_remote_copy(
            src_ref=sends[step].at[block],
            dst_ref=recvs[step].at[block],
            send_sem=ch_send.at[step],
            recv_sem=ch_recv.at[step, chunk],
            device_id={"chan": flip_bits(z, 1 << step)},
            device_id_type=MESH,
        )

    def correlate(slot, chunk):
        base = lax.rem(me + slot, n_tm) * count
        target, index = (vis, 0) if slot == 0 else (outbox, slot - 1)

        def one(k, carry):
            row = chunk * group + k
            a = pairs[0, base + row]
            e = pairs[1, base + row]
            ca, sa = cos_ref[a], sin_ref[a]
            ce, se = cos_ref[e], sin_ref[e]
            cos_diff = ca * ce + sa * se
            sin_diff = sa * ce - ca * se
            for period in range(periods):
                real = imag = None
                for m in range(samples):
                    ar, ai = x_ref[period, m, 0, a], x_ref[period, m, 1, a]
                    er, ei = x_ref[period, m, 0, e], x_ref[period, m, 1, e]
                    step_real = ar * er + ai * ei
                    step_imag = ai * er - ar * ei
                    real = step_real if real is None else real + step_real
                    imag = step_imag if imag is None else imag + step_imag
                real, imag = real.astype(f32), imag.astype(f32)
                both = jnp.concatenate(
                    [real * cos_diff + imag * sin_diff, imag * cos_diff - real * sin_diff], axis=0
                )
                target[index, row, period] = both.astype(bf16)
            return carry

        lax.fori_loop(0, group, one, 0)

    def outgoing(chunk):
        for slot in range(1, n_tm):
            correlate(slot, chunk)
            tm_copy(slot, chunk).start()

    def delay(chunk):
        for slot in range(1, n_tm):
            tm_copy(slot, chunk).wait_recv()

        def one(k, carry):
            row = chunk * group + k
            for slot in range(n_tm):
                for period in range(periods):
                    value = vis[slot, row, period]
                    section = jnp.dot(
                        first_ref[...],
                        jnp.concatenate([value, value], axis=0),
                        preferred_element_type=f32,
                    )
                    yr, yi = section[:outer], section[outer:]
                    tr = yr * tcos_ref[...] + yi * tsin_ref[...]
                    ti = yi * tcos_ref[...] - yr * tsin_ref[...]
                    place = slot * periods + period
                    twisted[place * outer : (place + 1) * outer, :inner] = tr.astype(bf16)
                    twisted[place * outer : (place + 1) * outer, inner:] = ti.astype(bf16)
            parts = []
            sign = jnp.where(
                lax.broadcasted_iota(jnp.int32, (outer, lanes), 1) < lanes // 2, 1.0, -1.0
            )
            for slot in range(n_tm):
                for period in range(periods):
                    place = slot * periods + period
                    both = jnp.dot(
                        twisted[place * outer : (place + 1) * outer],
                        last_ref[...],
                        preferred_element_type=f32,
                    )
                    value = both[:, :lanes] + both[:, lanes:]
                    turned = pltpu.roll(value, lanes // 2, 1) * sign
                    parts.append(((period - periods * slot) % rates, value, turned))
            for rate in range(rates):
                total = None
                for when, value, turned in parts:
                    angle = two_pi * (rate * when % rates) / rates
                    total = add_scaled(total, value, math.cos(angle))
                    total = add_scaled(total, turned, math.sin(angle))
                spec[rate] = total
            for q in range(rates):
                value = spec[flip_bits(z, q)]
                if q % 2 == 0:
                    keep[row, q // 2] = value
                else:
                    sends[0][row, q // 2] = value.astype(bf16)
            return carry

        lax.fori_loop(0, group, one, 0)
        chan_copy(0, chunk).start()

    def combine(step, chunk):
        chan_copy(step, chunk).wait_recv()

        def one(k, carry):
            row = chunk * group + k
            for j in range(recvs[step].shape[1]):
                total = keep[row, j << step] + recvs[step][row, j].astype(f32)
                if step == steps - 1:
                    turned = jnp.transpose(total)
                    half = lanes // 2
                    out_ref[row] = (turned[:half] ** 2 + turned[half:] ** 2) * scale
                elif j % 2 == 0:
                    keep[row, j << step] = total
                else:
                    sends[step + 1][row, j // 2] = total.astype(bf16)
            return carry

        lax.fori_loop(0, group, one, 0)
        if step < steps - 1:
            chan_copy(step + 1, chunk).start()

    for i in range(min(AHEAD, chunks)):
        outgoing(i)

    def round_trip(i, carry):
        @pl.when(i + AHEAD < chunks)
        def _():
            outgoing(i + AHEAD)

        @pl.when(i < chunks)
        def _():
            correlate(0, i)
            delay(i)

        for step in range(steps):
            lag = LAG * (step + 1)

            @pl.when((i >= lag) & (i - lag < chunks))
            def _():
                combine(step, i - lag)

        return carry

    lax.fori_loop(0, chunks + steps * LAG, round_trip, 0)

    for slot in range(1, n_tm):
        tm_copy(slot, 0, everything).wait_send()
    for step in range(steps):
        chan_copy(step, 0, everything).wait_send()


def fringe(n_tm, n_chan, pairs, tones, pcal_phase, samples):
    steps = n_chan.bit_length() - 1
    _, periods, taken, _, stations, width = samples.shape
    depth = width // INNER
    rowed = samples.reshape(periods, taken, 2, stations // SUB, SUB, width // LANES, LANES)
    rowed = rowed.transpose(0, 1, 2, 3, 5, 4, 6).reshape(periods, taken, 2, -1, LANES)
    rates = periods * n_tm
    count = pairs.shape[1] // n_tm
    group = max(g for g in range(1, GROUP + 1) if count % g == 0)
    chunks = count // group
    constants = tables(n_chan, depth)
    firsts, twist_cos, _, last = constants
    outer = twist_cos.shape[0]
    lanes = last.shape[1] // 2
    scale = 1.0 / (100.0 * taken * rates * n_chan * width)
    tile = (outer, lanes)
    boxes = [pltpu.VMEM((count, rates >> (s + 1)) + tile, bf16) for s in range(steps)]
    vmem = pl.BlockSpec(memory_space=pltpu.VMEM)
    stay = pl.BlockSpec(memory_space=pltpu.HBM)
    return pl.pallas_call(
        functools.partial(kernel, n_tm, n_chan, group, scale),
        out_shape=pltpu.VMEM((count, lanes // 2, outer), f32),
        in_specs=[pl.BlockSpec(memory_space=pltpu.SMEM)] + [stay] * 7,
        out_specs=vmem,
        scratch_shapes=[
            pltpu.VMEM((periods, taken, 2, width // LANES * stations, LANES), jnp.int32),
            pltpu.VMEM((periods, taken, 2, stations, depth, INNER), bf16),
            pltpu.VMEM(tones.shape, jnp.int32),
            pltpu.VMEM(pcal_phase.shape[1:], f32),
            pltpu.VMEM((stations, depth, INNER), f32),
            pltpu.VMEM((stations, depth, INNER), f32),
            pltpu.VMEM(firsts.shape[1:], bf16),
            pltpu.VMEM(twist_cos.shape, f32),
            pltpu.VMEM(twist_cos.shape, f32),
            pltpu.VMEM(last.shape, bf16),
            pltpu.VMEM((n_tm, count, periods, 2 * depth, INNER), bf16),
            pltpu.VMEM((n_tm - 1, count, periods, 2 * depth, INNER), bf16),
            pltpu.VMEM((rates * outer, 2 * INNER), bf16),
            pltpu.VMEM((rates,) + tile, f32),
            pltpu.VMEM((count, rates // 2) + tile, f32),
        ]
        + boxes
        + boxes
        + [
            pltpu.SemaphoreType.DMA((2,)),
            pltpu.SemaphoreType.DMA((periods,)),
            pltpu.SemaphoreType.DMA((len(constants),)),
            pltpu.SemaphoreType.DMA((n_tm - 1,)),
            pltpu.SemaphoreType.DMA((n_tm - 1, chunks)),
            pltpu.SemaphoreType.DMA((steps,)),
            pltpu.SemaphoreType.DMA((steps, chunks)),
        ],
        compiler_params=pltpu.CompilerParams(
            collective_id=0, has_side_effects=True, vmem_limit_bytes=57 << 20
        ),
        name="fringe",
    )(pairs, rowed, tones, pcal_phase, *(jnp.asarray(c) for c in constants))


def lending_tables(n_chan, depth, lent):
    firsts, twist_cos, twist_sin, last = tables(n_chan, depth)
    width = 2 * depth
    rows = np.concatenate([np.arange(lent), depth + np.arange(lent)])
    rest = np.concatenate([np.arange(lent, depth), depth + np.arange(lent, depth)])
    own, added = [], []
    for z in range(n_chan):
        high, low = firsts[z][:, :width], firsts[z][:, width:]
        own.append(np.concatenate([high, high, low], axis=1))
        high, low = firsts[z ^ 1][:, :width], firsts[z ^ 1][:, width:]
        added.append(
            np.concatenate(
                [high[:, rows], high[:, rows], low[:, rows], high[:, rest], low[:, rest]], axis=1
            )
        )
    both = np.concatenate([np.stack(own), np.stack(added)], axis=2)
    return both, twist_cos, twist_sin, last


def lending_kernel(n_tm, scale, names, *flat):
    ref = dict(zip(names, flat))
    out_ref, codes, x_ref, lent_x = ref["out"], ref["codes"], ref["x"], ref["lent_x"]
    vis, outbox, lent_vis, lent_box = ref["vis"], ref["outbox"], ref["lent_vis"], ref["lent_box"]
    waves, lent_waves, passed = ref["waves"], ref["lent_waves"], ref["passed"]
    twisted, keep, cross_out, cross_in = ref["twisted"], ref["keep"], ref["cross_out"], ref["cross_in"]
    first_ref, tcos_ref, tsin_ref, last_ref = ref["first"], ref["tcos"], ref["tsin"], ref["last"]
    pairs, tones = ref["pairs"], ref["tones"]

    periods, samples, _, stations, depth, inner = x_ref.shape
    lent = lent_x.shape[4]
    count = vis.shape[1]
    rates = periods * n_tm
    outer = tcos_ref.shape[0]
    lanes = last_ref.shape[1] // 2
    halves = inner // LANES
    own_width = 6 * depth
    me = lax.axis_index("tm")
    z = lax.axis_index("chan")
    buddy = flip_bits(z, 1)
    across = flip_bits(z, 3)
    is_end = lax.rem(z, 3) == 0
    is_inner = lax.rem(z, 3) != 0

    def start_all(copies):
        for copy in copies:
            copy.start()

    def wait_all(copies):
        for copy in copies:
            copy.wait()

    phases = [
        pltpu.make_async_copy(ref["tones_in"], tones, ref["phase_sem"].at[0]),
        pltpu.make_async_copy(ref["pcal_in"].at[0], ref["pcal"], ref["phase_sem"].at[1]),
    ]
    fetches = [
        pltpu.make_async_copy(ref["samples"].at[p], codes.at[p], ref["code_sem"].at[p])
        for p in range(periods)
    ]
    constants = [
        pltpu.make_async_copy(source, target, ref["table_sem"].at[i])
        for i, (source, target) in enumerate(
            [
                (ref["firsts"].at[z], first_ref),
                (ref["tcos_in"], tcos_ref),
                (ref["tsin_in"], tsin_ref),
                (ref["last_in"], last_ref),
            ]
        )
    ]
    start_all(phases + fetches + constants)

    barrier = pltpu.get_barrier_semaphore()
    for slot in range(1, n_tm):
        pl.semaphore_signal(
            barrier, inc=1, device_id={"tm": lax.rem(me + slot, n_tm)}, device_id_type=MESH
        )
    pl.semaphore_signal(barrier, inc=1, device_id={"chan": buddy}, device_id_type=MESH)

    @pl.when(is_inner)
    def _():
        pl.semaphore_signal(barrier, inc=1, device_id={"chan": across}, device_id_type=MESH)

    def station_tables(source, cos_ref, sin_ref):
        tall = cos_ref.shape[1]

        def one(station, carry):
            phase = ref["pcal"][pl.ds(station, 1), :]
            for turn, target in ((jnp.cos, cos_ref), (jnp.sin, sin_ref)):
                row = jnp.broadcast_to(turn(phase), (tall, LANES))
                for half in range(halves):
                    index = source[pl.ds(half, tall, stride=halves), :]
                    target[station, :, half * LANES : (half + 1) * LANES] = jnp.take_along_axis(
                        row, index, axis=1
                    )
            return carry

        lax.fori_loop(0, stations, one, 0)

    def lend(period):
        return pltpu.make_async_remote_copy(
            src_ref=x_ref.at[period, :, :, :, pl.ds(0, lent)],
            dst_ref=lent_x.at[period],
            send_sem=ref["lend_send"].at[period],
            recv_sem=ref["lend_recv"].at[period],
            device_id={"chan": buddy},
            device_id_type=MESH,
        )

    lend_tones = pltpu.make_async_remote_copy(
        src_ref=tones,
        dst_ref=ref["lent_tones"],
        send_sem=ref["lend_send"].at[periods],
        recv_sem=ref["lend_recv"].at[periods],
        device_id={"chan": buddy},
        device_id_type=MESH,
    )

    wait_all(phases)
    station_tables(tones, ref["cos"], ref["sin"])
    for period in range(periods):
        fetches[period].wait()

        def levels(station, carry):
            for m in range(samples):
                for part in range(2):
                    for half in range(halves):
                        start = lax.div(station, SUB) * (depth * halves * SUB) + half * SUB
                        code = codes[
                            period,
                            m,
                            part,
                            pl.ds(start + lax.rem(station, SUB), depth, stride=halves * SUB),
                            :,
                        ]
                        x_ref[
                            period, m, part, station, :, half * LANES : (half + 1) * LANES
                        ] = (2 * code - 3).astype(f32).astype(bf16)
            return carry

        lax.fori_loop(0, stations, levels, 0)
        if period == 0:

            @pl.when(is_end)
            def _():
                pl.semaphore_wait(barrier, n_tm)

            @pl.when(is_inner)
            def _():
                pl.semaphore_wait(barrier, n_tm + 1)

        @pl.when(is_end)
        def _():
            lend(period).start()

    @pl.when(is_end)
    def _():
        lend_tones.start()

    wait_all(constants)

    def tm_copy(slot, row, size=1):
        block = pl.ds(row, size)
        return pltpu.make_async_remote_copy(
            src_ref=outbox.at[slot - 1, block],
            dst_ref=vis.at[slot, block],
            send_sem=ref["tm_send"].at[slot - 1],
            recv_sem=ref["tm_recv"].at[slot - 1, row],
            device_id={"tm": lax.rem(me + slot, n_tm)},
            device_id_type=MESH,
        )

    def lent_copy(slot, row, size=1):
        block = pl.ds(row, size)
        return pltpu.make_async_remote_copy(
            src_ref=lent_box.at[slot - 1, block],
            dst_ref=lent_vis.at[slot, block],
            send_sem=ref["tm_lent_send"].at[slot - 1],
            recv_sem=ref["tm_lent_recv"].at[slot - 1, row],
            device_id={"tm": lax.rem(me + slot, n_tm)},
            device_id_type=MESH,
        )

    def pass_copy(row, size=1):
        block = pl.ds(row, size)
        return pltpu.make_async_remote_copy(
            src_ref=passed.at[block],
            dst_ref=passed.at[block],
            send_sem=ref["pass_send"],
            recv_sem=ref["pass_recv"].at[row],
            device_id={"chan": buddy},
            device_id_type=MESH,
        )

    def cross_copy(row, size=1):
        block = pl.ds(row, size)
        return pltpu.make_async_remote_copy(
            src_ref=cross_out.at[block],
            dst_ref=cross_in.at[block],
            send_sem=ref["cross_send"],
            recv_sem=ref["sum_recv"].at[row],
            device_id={"chan": across},
            device_id_type=MESH,
        )

    def back_copy(row, size=1):
        block = pl.ds(row, size)
        return pltpu.make_async_remote_copy(
            src_ref=keep.at[1, block],
            dst_ref=keep.at[1, block],
            send_sem=ref["back_send"],
            recv_sem=ref["sum_recv"].at[row],
            device_id={"chan": buddy},
            device_id_type=MESH,
        )

    def correlate(slot, row, voltage, cos_ref, sin_ref, target, index):
        place = lax.rem(me + slot, n_tm) * count + row
        a = pairs[0, place]
        e = pairs[1, place]
        ca, sa = cos_ref[a], sin_ref[a]
        ce, se = cos_ref[e], sin_ref[e]
        cos_diff = ca * ce + sa * se
        sin_diff = sa * ce - ca * se
        for period in range(periods):
            real = imag = None
            for m in range(samples):
                ar, ai = voltage[period, m, 0, a], voltage[period, m, 1, a]
                er, ei = voltage[period, m, 0, e], voltage[period, m, 1, e]
                step_real = ar * er + ai * ei
                step_imag = ai * er - ar * ei
                real = step_real if real is None else real + step_real
                imag = step_imag if imag is None else imag + step_imag
            real, imag = real.astype(f32), imag.astype(f32)
            both = jnp.concatenate(
                [real * cos_diff + imag * sin_diff, imag * cos_diff - real * sin_diff], axis=0
            )
            target[index, row, period] = both.astype(bf16)

    def own_visibility(slot, row):
        target, index = (vis, 0) if slot == 0 else (outbox, slot - 1)
        correlate(slot, row, x_ref, ref["cos"], ref["sin"], target, index)

    def lent_visibility(slot, row):
        target, index = (lent_vis, 0) if slot == 0 else (lent_box, slot - 1)
        correlate(slot, row, lent_x, ref["lent_cos"], ref["lent_sin"], target, index)

    def outgoing(row):
        for slot in range(1, n_tm):
            own_visibility(slot, row)
            tm_copy(slot, row).start()

    def lent_outgoing(row):
        for slot in range(1, n_tm):
            lent_visibility(slot, row)
            lent_copy(slot, row).start()

    def spectra(source, row, target):
        tall = target.shape[1] // 2
        parts = []
        for slot in range(n_tm):
            for period in range(periods):
                value = source[slot, row, period].astype(f32)
                parts.append(((period - periods * slot) % rates, value[:tall], value[tall:]))
        for rate in range(rates):
            real = imag = None
            for when, vr, vi in parts:
                angle = two_pi * (rate * when % rates) / rates
                c, s = math.cos(angle), math.sin(angle)
                real = add_scaled(add_scaled(real, vr, c), vi, s)
                imag = add_scaled(add_scaled(imag, vi, c), vr, -s)
            target[rate, :tall] = real
            target[rate, tall:] = imag

    def halves_of(value):
        high = value.astype(bf16)
        low = (value - high.astype(f32)).astype(bf16)
        return [high, low, high]

    def stage_one(place, columns, blocks):
        section = jnp.dot(
            columns, jnp.concatenate(blocks, axis=0), preferred_element_type=f32
        )
        yr, yi = section[:outer], section[outer:]
        tr = yr * tcos_ref[...] + yi * tsin_ref[...]
        ti = yi * tcos_ref[...] - yr * tsin_ref[...]
        twisted[place * outer : (place + 1) * outer, :inner] = tr.astype(bf16)
        twisted[place * outer : (place + 1) * outer, inner:] = ti.astype(bf16)

    def stage_two(place):
        both = jnp.dot(
            twisted[place * outer : (place + 1) * outer],
            last_ref[...],
            preferred_element_type=f32,
        )
        return both[:, :lanes] + both[:, lanes:]

    def finish(row, total):
        turned = jnp.transpose(total)
        half = lanes // 2
        out_ref[row] = (turned[:half] ** 2 + turned[half:] ** 2) * scale

    @pl.when(is_end)
    def _():
        def send_rows(row, carry):
            outgoing(row)
            return carry

        lax.fori_loop(0, count, send_rows, 0)
        for period in range(periods):
            lend(period).wait_send()
        lend_tones.wait_send()

        def one(row, carry):
            own_visibility(0, row)
            for slot in range(1, n_tm):
                tm_copy(slot, row).wait_recv()
            spectra(vis, row, waves)
            for q in range(1, rates):
                value = waves[flip_bits(z, q)]
                rest = jnp.concatenate([value[lent:depth], value[depth + lent :]], axis=0)
                passed[row, q - 1] = rest.astype(bf16)
            pass_copy(row).start()
            stage_one(0, first_ref[:, :own_width], halves_of(waves[z]))
            keep[0, row] = stage_two(0)
            return carry

        lax.fori_loop(0, count, one, 0)

        def close(row, carry):
            back_copy(row).wait_recv()
            finish(row, keep[0, row] + keep[1, row])
            return carry

        lax.fori_loop(0, count, close, 0)
        pass_copy(0, count).wait_send()

    @pl.when(is_inner)
    def _():
        def send_rows(row, carry):
            outgoing(row)
            return carry

        lax.fori_loop(0, min(FAR_AHEAD, count), send_rows, 0)
        for period in range(periods):
            lend(period).wait_recv()
        lend_tones.wait_recv()
        station_tables(ref["lent_tones"], ref["lent_cos"], ref["lent_sin"])

        def lend_rows(row, carry):
            lent_outgoing(row)
            return carry

        lax.fori_loop(0, min(LENT_AHEAD, count), lend_rows, 0)

        def one(row, carry):
            @pl.when(row + FAR_AHEAD < count)
            def _():
                outgoing(row + FAR_AHEAD)

            @pl.when(row + LENT_AHEAD < count)
            def _():
                lent_outgoing(row + LENT_AHEAD)

            @pl.when(row < count)
            def _():
                own_visibility(0, row)
                lent_visibility(0, row)
                for slot in range(1, n_tm):
                    tm_copy(slot, row).wait_recv()
                    lent_copy(slot, row).wait_recv()
                spectra(vis, row, waves)
                spectra(lent_vis, row, lent_waves)
                stage_one(1, first_ref[:, :own_width], halves_of(waves[buddy]))
                pass_copy(row).wait_recv()
                for q in range(rates):
                    if q != 1:
                        rate = flip_bits(z, q)
                        arrived = passed[row, (q ^ 1) - 1]
                        blocks = halves_of(waves[rate]) + halves_of(lent_waves[rate])
                        stage_one(q, first_ref[...], blocks + [arrived, arrived])
                keep[0, row] = stage_two(0)
                keep[1, row] = stage_two(1)
                cross_out[row, 0] = stage_two(3).astype(bf16)
                cross_out[row, 1] = stage_two(2).astype(bf16)
                cross_copy(row).start()

            @pl.when(row >= LAG)
            def _():
                late = row - LAG
                cross_copy(late).wait_recv()
                keep[1, late] = keep[1, late] + cross_in[late, 1].astype(f32)
                back_copy(late).start()
                finish(late, keep[0, late] + cross_in[late, 0].astype(f32))

            return carry

        lax.fori_loop(0, count + LAG, one, 0)
        for slot in range(1, n_tm):
            lent_copy(slot, 0, count).wait_send()
        cross_copy(0, count).wait_send()
        back_copy(0, count).wait_send()

    for slot in range(1, n_tm):
        tm_copy(slot, 0, count).wait_send()


def fringe_lending(n_tm, n_chan, pairs, tones, pcal_phase, samples):
    _, periods, taken, _, stations, width = samples.shape
    depth = width // INNER
    lent = min(LENT, depth // 2)
    rowed = samples.reshape(periods, taken, 2, stations // SUB, SUB, width // LANES, LANES)
    rowed = rowed.transpose(0, 1, 2, 3, 5, 4, 6).reshape(periods, taken, 2, -1, LANES)
    rates = periods * n_tm
    count = pairs.shape[1] // n_tm
    constants = lending_tables(n_chan, depth, lent)
    firsts, twist_cos, _, last = constants
    outer = twist_cos.shape[0]
    lanes = last.shape[1] // 2
    scale = 1.0 / (100.0 * taken * rates * n_chan * width)
    tile = (outer, lanes)
    dma = pltpu.SemaphoreType.DMA
    kept = {
        "codes": pltpu.VMEM((periods, taken, 2, width // LANES * stations, LANES), jnp.int32),
        "x": pltpu.VMEM((periods, taken, 2, stations, depth, INNER), bf16),
        "lent_x": pltpu.VMEM((periods, taken, 2, stations, lent, INNER), bf16),
        "tones": pltpu.VMEM(tones.shape, jnp.int32),
        "lent_tones": pltpu.VMEM(tones.shape, jnp.int32),
        "pcal": pltpu.VMEM(pcal_phase.shape[1:], f32),
        "cos": pltpu.VMEM((stations, depth, INNER), f32),
        "sin": pltpu.VMEM((stations, depth, INNER), f32),
        "lent_cos": pltpu.VMEM((stations, lent, INNER), f32),
        "lent_sin": pltpu.VMEM((stations, lent, INNER), f32),
        "first": pltpu.VMEM(firsts.shape[1:], bf16),
        "tcos": pltpu.VMEM(twist_cos.shape, f32),
        "tsin": pltpu.VMEM(twist_cos.shape, f32),
        "last": pltpu.VMEM(last.shape, bf16),
        "vis": pltpu.VMEM((n_tm, count, periods, 2 * depth, INNER), bf16),
        "outbox": pltpu.VMEM((n_tm - 1, count, periods, 2 * depth, INNER), bf16),
        "lent_vis": pltpu.VMEM((n_tm, count, periods, 2 * lent, INNER), bf16),
        "lent_box": pltpu.VMEM((n_tm - 1, count, periods, 2 * lent, INNER), bf16),
        "waves": pltpu.VMEM((rates, 2 * depth, INNER), f32),
        "lent_waves": pltpu.VMEM((rates, 2 * lent, INNER), f32),
        "passed": pltpu.VMEM((count, rates - 1, 2 * (depth - lent), INNER), bf16),
        "twisted": pltpu.VMEM((rates * outer, 2 * INNER), bf16),
        "keep": pltpu.VMEM((2, count) + tile, f32),
        "cross_out": pltpu.VMEM((count, 2) + tile, bf16),
        "cross_in": pltpu.VMEM((count, 2) + tile, bf16),
        "phase_sem": dma((2,)),
        "code_sem": dma((periods,)),
        "table_sem": dma((len(constants),)),
        "lend_send": dma((periods + 1,)),
        "lend_recv": dma((periods + 1,)),
        "tm_send": dma((n_tm - 1,)),
        "tm_recv": dma((n_tm - 1, count)),
        "tm_lent_send": dma((n_tm - 1,)),
        "tm_lent_recv": dma((n_tm - 1, count)),
        "pass_send": dma,
        "pass_recv": dma((count,)),
        "cross_send": dma,
        "back_send": dma,
        "sum_recv": dma((count,)),
    }
    given = ["pairs", "samples", "tones_in", "pcal_in", "firsts", "tcos_in", "tsin_in", "last_in"]
    vmem = pl.BlockSpec(memory_space=pltpu.VMEM)
    stay = pl.BlockSpec(memory_space=pltpu.HBM)
    return pl.pallas_call(
        functools.partial(lending_kernel, n_tm, scale, given + ["out"] + list(kept)),
        out_shape=pltpu.VMEM((count, lanes // 2, outer), f32),
        in_specs=[pl.BlockSpec(memory_space=pltpu.SMEM)] + [stay] * 7,
        out_specs=vmem,
        scratch_shapes=list(kept.values()),
        compiler_params=pltpu.CompilerParams(
            collective_id=0, has_side_effects=True, vmem_limit_bytes=57 << 20
        ),
        name="fringe_lending",
    )(pairs, rowed, tones, pcal_phase, *(jnp.asarray(c) for c in constants))


def shards(samples, pcal_phase, tone_index, baseline_pairs):
    n_chan = lax.axis_size("chan")
    search = fringe_lending if n_chan == 4 else fringe
    power = search(
        lax.axis_size("tm"),
        n_chan,
        baseline_pairs.T,
        tone_index.reshape(-1, LANES),
        pcal_phase,
        samples,
    )
    return power.reshape(1, 1, power.shape[0], ND)


def solution(mesh):
    placed = (
        P("pol", ("scan", "tm"), None, None, None, "chan"),
        P("pol", None, None),
        P("chan"),
        P(),
    )
    return jax.shard_map(
        shards,
        mesh=mesh,
        in_specs=placed,
        out_specs=P("pol", ("scan", "chan"), "tm", None),
        check_vma=False,
    )
```

```python
import functools
import math

import jax
import jax.numpy as jnp
import numpy as np
from jax import lax
from jax.experimental import pallas as pl
from jax.experimental.pallas import tpu as pltpu
from jax.sharding import PartitionSpec as P

S = 16
ND = 8192
LANES = 128
SUB = 8
INNER = 256
GROUP = 1
AHEAD = 2
LAG = 4
LENT = 8
FAR_AHEAD = 18
LENT_AHEAD = 13
EARLY = 1

two_pi = 2.0 * math.pi
f32, bf16 = jnp.float32, jnp.bfloat16
MESH = pl.DeviceIdType.MESH


def split_hi_lo(value):
    high = np.asarray(value, np.float32).astype(bf16)
    low = (np.asarray(value, np.float64) - high.astype(np.float64)).astype(np.float32).astype(bf16)
    return high, low


def phase_table(left, right, modulus):
    angles = two_pi * (np.outer(left, right) % modulus) / modulus
    return np.cos(angles), np.sin(angles)


def tables(n_chan, depth):
    channels = n_chan * depth * INNER
    outer = channels // INNER
    wide = ND // outer
    outer_axis = np.arange(outer)
    inner_axis = np.arange(INNER)
    firsts = []
    for z in range(n_chan):
        fc, fs = phase_table(outer_axis, z * depth + np.arange(depth), outer)
        both = np.concatenate(
            [np.concatenate([fc, fs], axis=1), np.concatenate([-fs, fc], axis=1)], axis=0
        )
        firsts.append(np.concatenate(split_hi_lo(both), axis=1))
    twist_cos, twist_sin = phase_table(outer_axis, inner_axis, channels)
    lc, ls = phase_table(inner_axis, np.arange(wide) - wide // 2, INNER)
    last = np.concatenate(
        [np.concatenate([lc, -ls], axis=1), np.concatenate([ls, lc], axis=1)], axis=0
    )
    last = np.concatenate(split_hi_lo(last), axis=1)
    return np.stack(firsts), twist_cos.astype(np.float32), twist_sin.astype(np.float32), last


def add_scaled(total, value, factor):
    if abs(factor) < 1e-9:
        return total
    if abs(factor - 1.0) < 1e-9:
        return value if total is None else total + value
    if abs(factor + 1.0) < 1e-9:
        return -value if total is None else total - value
    return value * factor if total is None else total + value * factor


def flip_bits(z, q):
    out, bit = z, 1
    while bit <= q:
        if q & bit:
            out = out + bit * (1 - 2 * lax.rem(lax.div(z, bit), 2))
        bit *= 2
    return out


def kernel(n_tm, n_chan, group, scale, *refs):
    steps = n_chan.bit_length() - 1
    (pairs, samples_ref, tones_in, pcal_in, firsts, *tables_in), refs = refs[:8], refs[8:]
    (out_ref, codes, x_ref, tones, pcal, cos_ref, sin_ref), refs = refs[:7], refs[7:]
    (first_ref, tcos_ref, tsin_ref, last_ref), refs = refs[:4], refs[4:]
    (vis, outbox, twisted, spec, keep), refs = refs[:5], refs[5:]
    sends, recvs = refs[:steps], refs[steps : 2 * steps]
    phase_sem, code_sem, table_sem, tm_send, tm_recv, ch_send, ch_recv = refs[2 * steps :]

    periods, samples, _, stations, depth, inner = x_ref.shape
    count = vis.shape[1]
    chunks = count // group
    rates = periods * n_tm
    outer = tcos_ref.shape[0]
    lanes = last_ref.shape[1] // 2
    halves = inner // LANES
    me = lax.axis_index("tm")
    z = lax.axis_index("chan")

    phases = [
        pltpu.make_async_copy(tones_in, tones, phase_sem.at[0]),
        pltpu.make_async_copy(pcal_in.at[0], pcal, phase_sem.at[1]),
    ]
    fetches = [
        pltpu.make_async_copy(samples_ref.at[period], codes.at[period], code_sem.at[period])
        for period in range(periods)
    ]
    for copy in phases + fetches:
        copy.start()
    constants = [
        pltpu.make_async_copy(source, target, table_sem.at[i])
        for i, (source, target) in enumerate(
            zip([firsts.at[z]] + tables_in, [first_ref, tcos_ref, tsin_ref, last_ref])
        )
    ]
    for copy in constants:
        copy.start()

    barrier = pltpu.get_barrier_semaphore()
    for slot in range(1, n_tm):
        pl.semaphore_signal(
            barrier, inc=1, device_id={"tm": lax.rem(me + slot, n_tm)}, device_id_type=MESH
        )
    for step in range(steps):
        pl.semaphore_signal(
            barrier, inc=1, device_id={"chan": flip_bits(z, 1 << step)}, device_id_type=MESH
        )

    def station_table(station, carry):
        phase = pcal[pl.ds(station, 1), :]
        for turn, target in ((jnp.cos, cos_ref), (jnp.sin, sin_ref)):
            row = jnp.broadcast_to(turn(phase), (depth, LANES))
            for half in range(halves):
                index = tones[pl.ds(half, depth, stride=halves), :]
                target[station, :, half * LANES : (half + 1) * LANES] = jnp.take_along_axis(
                    row, index, axis=1
                )
        return carry

    for copy in phases:
        copy.wait()
    lax.fori_loop(0, stations, station_table, 0)

    for period in range(periods):
        fetches[period].wait()

        def levels(station, carry):
            for m in range(samples):
                for part in range(2):
                    for half in range(halves):
                        start = lax.div(station, SUB) * (depth * halves * SUB) + half * SUB
                        code = codes[
                            period,
                            m,
                            part,
                            pl.ds(start + lax.rem(station, SUB), depth, stride=halves * SUB),
                            :,
                        ]
                        x_ref[
                            period, m, part, station, :, half * LANES : (half + 1) * LANES
                        ] = (2 * code - 3).astype(f32).astype(bf16)
            return carry

        lax.fori_loop(0, stations, levels, 0)
    for copy in constants:
        copy.wait()
    pl.semaphore_wait(barrier, n_tm - 1 + steps)

    def rows(chunk):
        return pl.ds(chunk * group, group)

    everything = pl.ds(0, count)

    def tm_copy(slot, chunk, block=None):
        block = rows(chunk) if block is None else block
        return pltpu.make_async_remote_copy(
            src_ref=outbox.at[slot - 1, block],
            dst_ref=vis.at[slot, block],
            send_sem=tm_send.at[slot - 1],
            recv_sem=tm_recv.at[slot - 1, chunk],
            device_id={"tm": lax.rem(me + slot, n_tm)},
            device_id_type=MESH,
        )

    def chan_copy(step, chunk, block=None):
        block = rows(chunk) if block is None else block
        return pltpu.make_async_remote_copy(
            src_ref=sends[step].at[block],
            dst_ref=recvs[step].at[block],
            send_sem=ch_send.at[step],
            recv_sem=ch_recv.at[step, chunk],
            device_id={"chan": flip_bits(z, 1 << step)},
            device_id_type=MESH,
        )

    def correlate(slot, chunk):
        base = lax.rem(me + slot, n_tm) * count
        target, index = (vis, 0) if slot == 0 else (outbox, slot - 1)

        def one(k, carry):
            row = chunk * group + k
            a = pairs[0, base + row]
            e = pairs[1, base + row]
            ca, sa = cos_ref[a], sin_ref[a]
            ce, se = cos_ref[e], sin_ref[e]
            cos_diff = ca * ce + sa * se
            sin_diff = sa * ce - ca * se
            for period in range(periods):
                real = imag = None
                for m in range(samples):
                    ar, ai = x_ref[period, m, 0, a], x_ref[period, m, 1, a]
                    er, ei = x_ref[period, m, 0, e], x_ref[period, m, 1, e]
                    step_real = ar * er + ai * ei
                    step_imag = ai * er - ar * ei
                    real = step_real if real is None else real + step_real
                    imag = step_imag if imag is None else imag + step_imag
                real, imag = real.astype(f32), imag.astype(f32)
                both = jnp.concatenate(
                    [real * cos_diff + imag * sin_diff, imag * cos_diff - real * sin_diff], axis=0
                )
                target[index, row, period] = both.astype(bf16)
            return carry

        lax.fori_loop(0, group, one, 0)

    def outgoing(chunk):
        for slot in range(1, n_tm):
            correlate(slot, chunk)
            tm_copy(slot, chunk).start()

    def delay(chunk):
        for slot in range(1, n_tm):
            tm_copy(slot, chunk).wait_recv()

        def one(k, carry):
            row = chunk * group + k
            for slot in range(n_tm):
                for period in range(periods):
                    value = vis[slot, row, period]
                    section = jnp.dot(
                        first_ref[...],
                        jnp.concatenate([value, value], axis=0),
                        preferred_element_type=f32,
                    )
                    yr, yi = section[:outer], section[outer:]
                    tr = yr * tcos_ref[...] + yi * tsin_ref[...]
                    ti = yi * tcos_ref[...] - yr * tsin_ref[...]
                    place = slot * periods + period
                    twisted[place * outer : (place + 1) * outer, :inner] = tr.astype(bf16)
                    twisted[place * outer : (place + 1) * outer, inner:] = ti.astype(bf16)
            parts = []
            sign = jnp.where(
                lax.broadcasted_iota(jnp.int32, (outer, lanes), 1) < lanes // 2, 1.0, -1.0
            )
            for slot in range(n_tm):
                for period in range(periods):
                    place = slot * periods + period
                    both = jnp.dot(
                        twisted[place * outer : (place + 1) * outer],
                        last_ref[...],
                        preferred_element_type=f32,
                    )
                    value = both[:, :lanes] + both[:, lanes:]
                    turned = pltpu.roll(value, lanes // 2, 1) * sign
                    parts.append(((period - periods * slot) % rates, value, turned))
            for rate in range(rates):
                total = None
                for when, value, turned in parts:
                    angle = two_pi * (rate * when % rates) / rates
                    total = add_scaled(total, value, math.cos(angle))
                    total = add_scaled(total, turned, math.sin(angle))
                spec[rate] = total
            for q in range(rates):
                value = spec[flip_bits(z, q)]
                if q % 2 == 0:
                    keep[row, q // 2] = value
                else:
                    sends[0][row, q // 2] = value.astype(bf16)
            return carry

        lax.fori_loop(0, group, one, 0)
        chan_copy(0, chunk).start()

    def combine(step, chunk):
        chan_copy(step, chunk).wait_recv()

        def one(k, carry):
            row = chunk * group + k
            for j in range(recvs[step].shape[1]):
                total = keep[row, j << step] + recvs[step][row, j].astype(f32)
                if step == steps - 1:
                    turned = jnp.transpose(total)
                    half = lanes // 2
                    out_ref[row] = (turned[:half] ** 2 + turned[half:] ** 2) * scale
                elif j % 2 == 0:
                    keep[row, j << step] = total
                else:
                    sends[step + 1][row, j // 2] = total.astype(bf16)
            return carry

        lax.fori_loop(0, group, one, 0)
        if step < steps - 1:
            chan_copy(step + 1, chunk).start()

    for i in range(min(AHEAD, chunks)):
        outgoing(i)

    def round_trip(i, carry):
        @pl.when(i + AHEAD < chunks)
        def _():
            outgoing(i + AHEAD)

        @pl.when(i < chunks)
        def _():
            correlate(0, i)
            delay(i)

        for step in range(steps):
            lag = LAG * (step + 1)

            @pl.when((i >= lag) & (i - lag < chunks))
            def _():
                combine(step, i - lag)

        return carry

    lax.fori_loop(0, chunks + steps * LAG, round_trip, 0)

    for slot in range(1, n_tm):
        tm_copy(slot, 0, everything).wait_send()
    for step in range(steps):
        chan_copy(step, 0, everything).wait_send()


def fringe(n_tm, n_chan, pairs, tones, pcal_phase, samples):
    steps = n_chan.bit_length() - 1
    _, periods, taken, _, stations, width = samples.shape
    depth = width // INNER
    rowed = samples.reshape(periods, taken, 2, stations // SUB, SUB, width // LANES, LANES)
    rowed = rowed.transpose(0, 1, 2, 3, 5, 4, 6).reshape(periods, taken, 2, -1, LANES)
    rates = periods * n_tm
    count = pairs.shape[1] // n_tm
    group = max(g for g in range(1, GROUP + 1) if count % g == 0)
    chunks = count // group
    constants = tables(n_chan, depth)
    firsts, twist_cos, _, last = constants
    outer = twist_cos.shape[0]
    lanes = last.shape[1] // 2
    scale = 1.0 / (100.0 * taken * rates * n_chan * width)
    tile = (outer, lanes)
    boxes = [pltpu.VMEM((count, rates >> (s + 1)) + tile, bf16) for s in range(steps)]
    vmem = pl.BlockSpec(memory_space=pltpu.VMEM)
    stay = pl.BlockSpec(memory_space=pltpu.HBM)
    return pl.pallas_call(
        functools.partial(kernel, n_tm, n_chan, group, scale),
        out_shape=pltpu.VMEM((count, lanes // 2, outer), f32),
        in_specs=[pl.BlockSpec(memory_space=pltpu.SMEM)] + [stay] * 7,
        out_specs=vmem,
        scratch_shapes=[
            pltpu.VMEM((periods, taken, 2, width // LANES * stations, LANES), jnp.int32),
            pltpu.VMEM((periods, taken, 2, stations, depth, INNER), bf16),
            pltpu.VMEM(tones.shape, jnp.int32),
            pltpu.VMEM(pcal_phase.shape[1:], f32),
            pltpu.VMEM((stations, depth, INNER), f32),
            pltpu.VMEM((stations, depth, INNER), f32),
            pltpu.VMEM(firsts.shape[1:], bf16),
            pltpu.VMEM(twist_cos.shape, f32),
            pltpu.VMEM(twist_cos.shape, f32),
            pltpu.VMEM(last.shape, bf16),
            pltpu.VMEM((n_tm, count, periods, 2 * depth, INNER), bf16),
            pltpu.VMEM((n_tm - 1, count, periods, 2 * depth, INNER), bf16),
            pltpu.VMEM((rates * outer, 2 * INNER), bf16),
            pltpu.VMEM((rates,) + tile, f32),
            pltpu.VMEM((count, rates // 2) + tile, f32),
        ]
        + boxes
        + boxes
        + [
            pltpu.SemaphoreType.DMA((2,)),
            pltpu.SemaphoreType.DMA((periods,)),
            pltpu.SemaphoreType.DMA((len(constants),)),
            pltpu.SemaphoreType.DMA((n_tm - 1,)),
            pltpu.SemaphoreType.DMA((n_tm - 1, chunks)),
            pltpu.SemaphoreType.DMA((steps,)),
            pltpu.SemaphoreType.DMA((steps, chunks)),
        ],
        compiler_params=pltpu.CompilerParams(
            collective_id=0, has_side_effects=True, vmem_limit_bytes=57 << 20
        ),
        name="fringe",
    )(pairs, rowed, tones, pcal_phase, *(jnp.asarray(c) for c in constants))


def lending_tables(n_chan, depth, lent):
    firsts, twist_cos, twist_sin, last = tables(n_chan, depth)
    width = 2 * depth
    rows = np.concatenate([np.arange(lent), depth + np.arange(lent)])
    rest = np.concatenate([np.arange(lent, depth), depth + np.arange(lent, depth)])
    own, added = [], []
    for z in range(n_chan):
        high, low = firsts[z][:, :width], firsts[z][:, width:]
        own.append(np.concatenate([high, high, low], axis=1))
        high, low = firsts[z ^ 1][:, :width], firsts[z ^ 1][:, width:]
        added.append(
            np.concatenate(
                [high[:, rows], high[:, rows], low[:, rows], high[:, rest], low[:, rest]], axis=1
            )
        )
    both = np.concatenate([np.stack(own), np.stack(added)], axis=2)
    return both, twist_cos, twist_sin, last


def lending_kernel(n_tm, scale, names, *flat):
    ref = dict(zip(names, flat))
    out_ref, codes, x_ref, lent_x = ref["out"], ref["codes"], ref["x"], ref["lent_x"]
    vis, outbox, lent_vis, lent_box = ref["vis"], ref["outbox"], ref["lent_vis"], ref["lent_box"]
    waves, lent_waves, passed = ref["waves"], ref["lent_waves"], ref["passed"]
    twisted, keep, home_out = ref["twisted"], ref["keep"], ref["home_out"]
    cross_out, sums_in = ref["cross_out"], ref["sums_in"]
    first_ref, tcos_ref, tsin_ref, last_ref = ref["first"], ref["tcos"], ref["tsin"], ref["last"]
    pairs, tones = ref["pairs"], ref["tones"]

    periods, samples, _, stations, depth, inner = x_ref.shape
    lent = lent_x.shape[4]
    count = vis.shape[1]
    rates = periods * n_tm
    outer = tcos_ref.shape[0]
    lanes = last_ref.shape[1] // 2
    halves = inner // LANES
    own_width = 6 * depth
    me = lax.axis_index("tm")
    z = lax.axis_index("chan")
    buddy = flip_bits(z, 1)
    across, far = flip_bits(z, 3), flip_bits(z, 2)
    is_end = lax.rem(z, 3) == 0
    is_inner = lax.rem(z, 3) != 0

    def start_all(copies):
        for copy in copies:
            copy.start()

    def wait_all(copies):
        for copy in copies:
            copy.wait()

    phases = [
        pltpu.make_async_copy(ref["tones_in"], tones, ref["phase_sem"].at[0]),
        pltpu.make_async_copy(ref["pcal_in"].at[0], ref["pcal"], ref["phase_sem"].at[1]),
    ]
    fetches = [
        pltpu.make_async_copy(ref["samples"].at[p], codes.at[p], ref["code_sem"].at[p])
        for p in range(periods)
    ]
    constants = [
        pltpu.make_async_copy(source, target, ref["table_sem"].at[i])
        for i, (source, target) in enumerate(
            [
                (ref["firsts"].at[z], first_ref),
                (ref["tcos_in"], tcos_ref),
                (ref["tsin_in"], tsin_ref),
                (ref["last_in"], last_ref),
            ]
        )
    ]
    start_all(phases + fetches + constants)

    barrier = pltpu.get_barrier_semaphore()
    for slot in range(1, n_tm):
        pl.semaphore_signal(
            barrier, inc=1, device_id={"tm": lax.rem(me + slot, n_tm)}, device_id_type=MESH
        )
    for other in (buddy, far):
        pl.semaphore_signal(barrier, inc=1, device_id={"chan": other}, device_id_type=MESH)

    @pl.when(is_inner)
    def _():
        pl.semaphore_signal(barrier, inc=1, device_id={"chan": across}, device_id_type=MESH)

    def station_tables(source, cos_ref, sin_ref):
        tall = cos_ref.shape[1]

        def one(station, carry):
            phase = ref["pcal"][pl.ds(station, 1), :]
            for turn, target in ((jnp.cos, cos_ref), (jnp.sin, sin_ref)):
                row = jnp.broadcast_to(turn(phase), (tall, LANES))
                for half in range(halves):
                    index = source[pl.ds(half, tall, stride=halves), :]
                    target[station, :, half * LANES : (half + 1) * LANES] = jnp.take_along_axis(
                        row, index, axis=1
                    )
            return carry

        lax.fori_loop(0, stations, one, 0)

    def lend(period):
        return pltpu.make_async_remote_copy(
            src_ref=x_ref.at[period, :, :, :, pl.ds(0, lent)],
            dst_ref=lent_x.at[period],
            send_sem=ref["lend_send"].at[period],
            recv_sem=ref["lend_recv"].at[period],
            device_id={"chan": buddy},
            device_id_type=MESH,
        )

    lend_tones = pltpu.make_async_remote_copy(
        src_ref=tones,
        dst_ref=ref["lent_tones"],
        send_sem=ref["lend_send"].at[periods],
        recv_sem=ref["lend_recv"].at[periods],
        device_id={"chan": buddy},
        device_id_type=MESH,
    )

    wait_all(phases)
    station_tables(tones, ref["cos"], ref["sin"])
    for period in range(periods):
        fetches[period].wait()

        def levels(station, carry):
            for m in range(samples):
                for part in range(2):
                    for half in range(halves):
                        start = lax.div(station, SUB) * (depth * halves * SUB) + half * SUB
                        code = codes[
                            period,
                            m,
                            part,
                            pl.ds(start + lax.rem(station, SUB), depth, stride=halves * SUB),
                            :,
                        ]
                        x_ref[
                            period, m, part, station, :, half * LANES : (half + 1) * LANES
                        ] = (2 * code - 3).astype(f32).astype(bf16)
            return carry

        lax.fori_loop(0, stations, levels, 0)
        if period == 0:

            @pl.when(is_end)
            def _():
                pl.semaphore_wait(barrier, n_tm + 1)
                lend_tones.start()

            @pl.when(is_inner)
            def _():
                pl.semaphore_wait(barrier, n_tm + 2)

        @pl.when(is_end)
        def _():
            lend(period).start()

    wait_all(constants)

    def tm_copy(slot, row, size=1):
        block = pl.ds(row, size)
        return pltpu.make_async_remote_copy(
            src_ref=outbox.at[slot - 1, block],
            dst_ref=vis.at[slot, block],
            send_sem=ref["tm_send"].at[slot - 1],
            recv_sem=ref["tm_recv"].at[slot - 1, row],
            device_id={"tm": lax.rem(me + slot, n_tm)},
            device_id_type=MESH,
        )

    def lent_copy(slot, row, size=1):
        block = pl.ds(row, size)
        return pltpu.make_async_remote_copy(
            src_ref=lent_box.at[slot - 1, block],
            dst_ref=lent_vis.at[slot, block],
            send_sem=ref["tm_lent_send"].at[slot - 1],
            recv_sem=ref["tm_lent_recv"].at[slot - 1, row],
            device_id={"tm": lax.rem(me + slot, n_tm)},
            device_id_type=MESH,
        )

    def pass_copy(row, size=1):
        block = pl.ds(row, size)
        return pltpu.make_async_remote_copy(
            src_ref=passed.at[block],
            dst_ref=passed.at[block],
            send_sem=ref["pass_send"],
            recv_sem=ref["pass_recv"].at[row],
            device_id={"chan": buddy},
            device_id_type=MESH,
        )

    def sum_copy(index, row):
        block = pl.ds(row, 1)
        return pltpu.make_async_remote_copy(
            src_ref=cross_out.at[index, block],
            dst_ref=sums_in.at[0, block],
            send_sem=ref["cross_send"],
            recv_sem=ref["sum_recv"].at[row],
            device_id={"chan": far if index else across},
            device_id_type=MESH,
        )

    def home_copy(row, size=1):
        block = pl.ds(row, size)
        return pltpu.make_async_remote_copy(
            src_ref=home_out.at[block],
            dst_ref=sums_in.at[1, block],
            send_sem=ref["home_send"],
            recv_sem=ref["pass_recv"].at[row],
            device_id={"chan": buddy},
            device_id_type=MESH,
        )

    cross_drain = pltpu.make_async_copy(cross_out, cross_out, ref["cross_send"])

    def correlate(slot, row, voltage, cos_ref, sin_ref, target, index):
        place = lax.rem(me + slot, n_tm) * count + row
        a = pairs[0, place]
        e = pairs[1, place]
        ca, sa = cos_ref[a], sin_ref[a]
        ce, se = cos_ref[e], sin_ref[e]
        cos_diff = ca * ce + sa * se
        sin_diff = sa * ce - ca * se
        for period in range(periods):
            real = imag = None
            for m in range(samples):
                ar, ai = voltage[period, m, 0, a], voltage[period, m, 1, a]
                er, ei = voltage[period, m, 0, e], voltage[period, m, 1, e]
                step_real = ar * er + ai * ei
                step_imag = ai * er - ar * ei
                real = step_real if real is None else real + step_real
                imag = step_imag if imag is None else imag + step_imag
            real, imag = real.astype(f32), imag.astype(f32)
            both = jnp.concatenate(
                [real * cos_diff + imag * sin_diff, imag * cos_diff - real * sin_diff], axis=0
            )
            target[index, row, period] = both.astype(bf16)

    def own_visibility(slot, row):
        target, index = (vis, 0) if slot == 0 else (outbox, slot - 1)
        correlate(slot, row, x_ref, ref["cos"], ref["sin"], target, index)

    def lent_visibility(slot, row):
        target, index = (lent_vis, 0) if slot == 0 else (lent_box, slot - 1)
        correlate(slot, row, lent_x, ref["lent_cos"], ref["lent_sin"], target, index)

    def outgoing(row):
        for slot in range(1, n_tm):
            own_visibility(slot, row)
            tm_copy(slot, row).start()

    def lent_outgoing(row):
        for slot in range(1, n_tm):
            lent_visibility(slot, row)
            lent_copy(slot, row).start()

    def spectra(source, row, target):
        tall = target.shape[1] // 2
        parts = []
        for slot in range(n_tm):
            for period in range(periods):
                value = source[slot, row, period].astype(f32)
                parts.append(((period - periods * slot) % rates, value[:tall], value[tall:]))
        for rate in range(rates):
            real = imag = None
            for when, vr, vi in parts:
                angle = two_pi * (rate * when % rates) / rates
                c, s = math.cos(angle), math.sin(angle)
                real = add_scaled(add_scaled(real, vr, c), vi, s)
                imag = add_scaled(add_scaled(imag, vi, c), vr, -s)
            target[rate, :tall] = real
            target[rate, tall:] = imag

    def halves_of(value):
        high = value.astype(bf16)
        low = (value - high.astype(f32)).astype(bf16)
        return [high, low, high]

    def stage_one(place, columns, blocks):
        section = jnp.dot(
            columns, jnp.concatenate(blocks, axis=0), preferred_element_type=f32
        )
        yr, yi = section[:outer], section[outer:]
        tr = yr * tcos_ref[...] + yi * tsin_ref[...]
        ti = yi * tcos_ref[...] - yr * tsin_ref[...]
        twisted[place * outer : (place + 1) * outer, :inner] = tr.astype(bf16)
        twisted[place * outer : (place + 1) * outer, inner:] = ti.astype(bf16)

    def stage_two(place):
        both = jnp.dot(
            twisted[place * outer : (place + 1) * outer],
            last_ref[...],
            preferred_element_type=f32,
        )
        return both[:, :lanes] + both[:, lanes:]

    def finish(row, total):
        turned = jnp.transpose(total)
        half = lanes // 2
        out_ref[row] = (turned[:half] ** 2 + turned[half:] ** 2) * scale

    @pl.when(is_end)
    def _():
        def send_rows(row, carry):
            outgoing(row)
            return carry

        lax.fori_loop(0, count, send_rows, 0)

        def one(row, carry):
            own_visibility(0, row)
            for slot in range(1, n_tm):
                tm_copy(slot, row).wait_recv()
            spectra(vis, row, waves)
            for q in range(1, rates):
                value = waves[flip_bits(z, q)]
                rest = jnp.concatenate([value[lent:depth], value[depth + lent :]], axis=0)
                passed[row, q - 1] = rest.astype(bf16)
            pass_copy(row).start()
            stage_one(0, first_ref[:, :own_width], halves_of(waves[z]))
            keep[row] = stage_two(0)
            return carry

        lax.fori_loop(0, min(EARLY, count), one, 0)
        lend_tones.wait_send()
        for period in range(periods):
            lend(period).wait_send()
        lax.fori_loop(min(EARLY, count), count, one, 0)

        def close(row, carry):
            home_copy(row).wait_recv()
            sum_copy(1, row).wait_recv()
            finish(row, keep[row] + sums_in[0, row].astype(f32) + sums_in[1, row].astype(f32))
            return carry

        lax.fori_loop(0, count, close, 0)
        pass_copy(0, count).wait_send()

    @pl.when(is_inner)
    def _():
        def send_rows(row, carry):
            outgoing(row)
            return carry

        lax.fori_loop(0, min(FAR_AHEAD, count), send_rows, 0)
        lend_tones.wait_recv()
        station_tables(ref["lent_tones"], ref["lent_cos"], ref["lent_sin"])
        for period in range(periods):
            lend(period).wait_recv()

        def lend_rows(row, carry):
            lent_outgoing(row)
            return carry

        lax.fori_loop(0, min(LENT_AHEAD, count), lend_rows, 0)

        def one(row, carry):
            @pl.when(row + FAR_AHEAD < count)
            def _():
                outgoing(row + FAR_AHEAD)

            @pl.when(row + LENT_AHEAD < count)
            def _():
                lent_outgoing(row + LENT_AHEAD)

            @pl.when(row < count)
            def _():
                own_visibility(0, row)
                lent_visibility(0, row)
                for slot in range(1, n_tm):
                    tm_copy(slot, row).wait_recv()
                spectra(vis, row, waves)
                for slot in range(1, n_tm):
                    lent_copy(slot, row).wait_recv()
                spectra(lent_vis, row, lent_waves)
                stage_one(1, first_ref[:, :own_width], halves_of(waves[buddy]))
                pass_copy(row).wait_recv()
                for q in range(rates):
                    if q != 1:
                        rate = flip_bits(z, q)
                        arrived = passed[row, (q ^ 1) - 1]
                        blocks = halves_of(waves[rate]) + halves_of(lent_waves[rate])
                        stage_one(q, first_ref[...], blocks + [arrived, arrived])
                keep[row] = stage_two(0)
                home_out[row] = stage_two(1).astype(bf16)
                cross_out[1, row] = stage_two(2).astype(bf16)
                cross_out[0, row] = stage_two(3).astype(bf16)
                sum_copy(1, row).start()
                sum_copy(0, row).start()
                home_copy(row).start()

            @pl.when(row >= LAG)
            def _():
                late = row - LAG
                sum_copy(0, late).wait_recv()
                finish(late, keep[late] + sums_in[0, late].astype(f32))

            return carry

        lax.fori_loop(0, count + LAG, one, 0)
        for slot in range(1, n_tm):
            lent_copy(slot, 0, count).wait_send()
        cross_drain.wait()
        home_copy(0, count).wait_send()

    for slot in range(1, n_tm):
        tm_copy(slot, 0, count).wait_send()


def fringe_lending(n_tm, n_chan, pairs, tones, pcal_phase, samples):
    _, periods, taken, _, stations, width = samples.shape
    depth = width // INNER
    lent = min(LENT, depth // 2)
    rowed = samples.reshape(periods, taken, 2, stations // SUB, SUB, width // LANES, LANES)
    rowed = rowed.transpose(0, 1, 2, 3, 5, 4, 6).reshape(periods, taken, 2, -1, LANES)
    rates = periods * n_tm
    count = pairs.shape[1] // n_tm
    constants = lending_tables(n_chan, depth, lent)
    firsts, twist_cos, _, last = constants
    outer = twist_cos.shape[0]
    lanes = last.shape[1] // 2
    scale = 1.0 / (100.0 * taken * rates * n_chan * width)
    tile = (outer, lanes)
    dma = pltpu.SemaphoreType.DMA
    kept = {
        "codes": pltpu.VMEM((periods, taken, 2, width // LANES * stations, LANES), jnp.int32),
        "x": pltpu.VMEM((periods, taken, 2, stations, depth, INNER), bf16),
        "lent_x": pltpu.VMEM((periods, taken, 2, stations, lent, INNER), bf16),
        "tones": pltpu.VMEM(tones.shape, jnp.int32),
        "lent_tones": pltpu.VMEM(tones.shape, jnp.int32),
        "pcal": pltpu.VMEM(pcal_phase.shape[1:], f32),
        "cos": pltpu.VMEM((stations, depth, INNER), f32),
        "sin": pltpu.VMEM((stations, depth, INNER), f32),
        "lent_cos": pltpu.VMEM((stations, lent, INNER), f32),
        "lent_sin": pltpu.VMEM((stations, lent, INNER), f32),
        "first": pltpu.VMEM(firsts.shape[1:], bf16),
        "tcos": pltpu.VMEM(twist_cos.shape, f32),
        "tsin": pltpu.VMEM(twist_cos.shape, f32),
        "last": pltpu.VMEM(last.shape, bf16),
        "vis": pltpu.VMEM((n_tm, count, periods, 2 * depth, INNER), bf16),
        "outbox": pltpu.VMEM((n_tm - 1, count, periods, 2 * depth, INNER), bf16),
        "lent_vis": pltpu.VMEM((n_tm, count, periods, 2 * lent, INNER), bf16),
        "lent_box": pltpu.VMEM((n_tm - 1, count, periods, 2 * lent, INNER), bf16),
        "waves": pltpu.VMEM((rates, 2 * depth, INNER), f32),
        "lent_waves": pltpu.VMEM((rates, 2 * lent, INNER), f32),
        "passed": pltpu.VMEM((count, rates - 1, 2 * (depth - lent), INNER), bf16),
        "twisted": pltpu.VMEM((rates * outer, 2 * INNER), bf16),
        "keep": pltpu.VMEM((count,) + tile, f32),
        "home_out": pltpu.VMEM((count,) + tile, bf16),
        "cross_out": pltpu.VMEM((2, count) + tile, bf16),
        "sums_in": pltpu.VMEM((2, count) + tile, bf16),
        "phase_sem": dma((2,)),
        "code_sem": dma((periods,)),
        "table_sem": dma((len(constants),)),
        "lend_send": dma((periods + 1,)),
        "lend_recv": dma((periods + 1,)),
        "tm_send": dma((n_tm - 1,)),
        "tm_recv": dma((n_tm - 1, count)),
        "tm_lent_send": dma((n_tm - 1,)),
        "tm_lent_recv": dma((n_tm - 1, count)),
        "pass_send": dma,
        "pass_recv": dma((count,)),
        "cross_send": dma,
        "home_send": dma,
        "sum_recv": dma((count,)),
    }
    given = ["pairs", "samples", "tones_in", "pcal_in", "firsts", "tcos_in", "tsin_in", "last_in"]
    vmem = pl.BlockSpec(memory_space=pltpu.VMEM)
    stay = pl.BlockSpec(memory_space=pltpu.HBM)
    return pl.pallas_call(
        functools.partial(lending_kernel, n_tm, scale, given + ["out"] + list(kept)),
        out_shape=pltpu.VMEM((count, lanes // 2, outer), f32),
        in_specs=[pl.BlockSpec(memory_space=pltpu.SMEM)] + [stay] * 7,
        out_specs=vmem,
        scratch_shapes=list(kept.values()),
        compiler_params=pltpu.CompilerParams(
            collective_id=0, has_side_effects=True, vmem_limit_bytes=57 << 20
        ),
        name="fringe_lending",
    )(pairs, rowed, tones, pcal_phase, *(jnp.asarray(c) for c in constants))


def shards(samples, pcal_phase, tone_index, baseline_pairs):
    n_chan = lax.axis_size("chan")
    search = fringe_lending if n_chan == 4 else fringe
    power = search(
        lax.axis_size("tm"),
        n_chan,
        baseline_pairs.T,
        tone_index.reshape(-1, LANES),
        pcal_phase,
        samples,
    )
    return power.reshape(1, 1, power.shape[0], ND)


def solution(mesh):
    placed = (
        P("pol", ("scan", "tm"), None, None, None, "chan"),
        P("pol", None, None),
        P("chan"),
        P(),
    )
    return jax.shard_map(
        shards,
        mesh=mesh,
        in_specs=placed,
        out_specs=P("pol", ("scan", "chan"), "tm", None),
        check_vma=False,
    )
```

```python
import functools
import math

import jax
import jax.numpy as jnp
import numpy as np
from jax import lax
from jax.experimental import pallas as pl
from jax.experimental.pallas import tpu as pltpu
from jax.sharding import PartitionSpec as P

S = 16
ND = 8192
LANES = 128
SUB = 8
INNER = 256
GROUP = 1
AHEAD = 2
LAG = 4
LENT = 8
FAR_AHEAD = 18
LENT_AHEAD = 14
EARLY = 1

two_pi = 2.0 * math.pi
f32, bf16 = jnp.float32, jnp.bfloat16
MESH = pl.DeviceIdType.MESH


def split_hi_lo(value):
    high = np.asarray(value, np.float32).astype(bf16)
    low = (np.asarray(value, np.float64) - high.astype(np.float64)).astype(np.float32).astype(bf16)
    return high, low


def phase_table(left, right, modulus):
    angles = two_pi * (np.outer(left, right) % modulus) / modulus
    return np.cos(angles), np.sin(angles)


def tables(n_chan, depth):
    channels = n_chan * depth * INNER
    outer = channels // INNER
    wide = ND // outer
    outer_axis = np.arange(outer)
    inner_axis = np.arange(INNER)
    firsts = []
    for z in range(n_chan):
        fc, fs = phase_table(outer_axis, z * depth + np.arange(depth), outer)
        both = np.concatenate(
            [np.concatenate([fc, fs], axis=1), np.concatenate([-fs, fc], axis=1)], axis=0
        )
        firsts.append(np.concatenate(split_hi_lo(both), axis=1))
    twist_cos, twist_sin = phase_table(outer_axis, inner_axis, channels)
    lc, ls = phase_table(inner_axis, np.arange(wide) - wide // 2, INNER)
    last = np.concatenate(
        [np.concatenate([lc, -ls], axis=1), np.concatenate([ls, lc], axis=1)], axis=0
    )
    last = np.concatenate(split_hi_lo(last), axis=1)
    return np.stack(firsts), twist_cos.astype(np.float32), twist_sin.astype(np.float32), last


def add_scaled(total, value, factor):
    if abs(factor) < 1e-9:
        return total
    if abs(factor - 1.0) < 1e-9:
        return value if total is None else total + value
    if abs(factor + 1.0) < 1e-9:
        return -value if total is None else total - value
    return value * factor if total is None else total + value * factor


def flip_bits(z, q):
    out, bit = z, 1
    while bit <= q:
        if q & bit:
            out = out + bit * (1 - 2 * lax.rem(lax.div(z, bit), 2))
        bit *= 2
    return out


def kernel(n_tm, n_chan, group, scale, *refs):
    steps = n_chan.bit_length() - 1
    (pairs, samples_ref, tones_in, pcal_in, firsts, *tables_in), refs = refs[:8], refs[8:]
    (out_ref, codes, x_ref, tones, pcal, cos_ref, sin_ref), refs = refs[:7], refs[7:]
    (first_ref, tcos_ref, tsin_ref, last_ref), refs = refs[:4], refs[4:]
    (vis, outbox, twisted, spec, keep), refs = refs[:5], refs[5:]
    sends, recvs = refs[:steps], refs[steps : 2 * steps]
    phase_sem, code_sem, table_sem, tm_send, tm_recv, ch_send, ch_recv = refs[2 * steps :]

    periods, samples, _, stations, depth, inner = x_ref.shape
    count = vis.shape[1]
    chunks = count // group
    rates = periods * n_tm
    outer = tcos_ref.shape[0]
    lanes = last_ref.shape[1] // 2
    halves = inner // LANES
    me = lax.axis_index("tm")
    z = lax.axis_index("chan")

    phases = [
        pltpu.make_async_copy(tones_in, tones, phase_sem.at[0]),
        pltpu.make_async_copy(pcal_in.at[0], pcal, phase_sem.at[1]),
    ]
    fetches = [
        pltpu.make_async_copy(samples_ref.at[period], codes.at[period], code_sem.at[period])
        for period in range(periods)
    ]
    for copy in phases + fetches:
        copy.start()
    constants = [
        pltpu.make_async_copy(source, target, table_sem.at[i])
        for i, (source, target) in enumerate(
            zip([firsts.at[z]] + tables_in, [first_ref, tcos_ref, tsin_ref, last_ref])
        )
    ]
    for copy in constants:
        copy.start()

    barrier = pltpu.get_barrier_semaphore()
    for slot in range(1, n_tm):
        pl.semaphore_signal(
            barrier, inc=1, device_id={"tm": lax.rem(me + slot, n_tm)}, device_id_type=MESH
        )
    for step in range(steps):
        pl.semaphore_signal(
            barrier, inc=1, device_id={"chan": flip_bits(z, 1 << step)}, device_id_type=MESH
        )

    def station_table(station, carry):
        phase = pcal[pl.ds(station, 1), :]
        for turn, target in ((jnp.cos, cos_ref), (jnp.sin, sin_ref)):
            row = jnp.broadcast_to(turn(phase), (depth, LANES))
            for half in range(halves):
                index = tones[pl.ds(half, depth, stride=halves), :]
                target[station, :, half * LANES : (half + 1) * LANES] = jnp.take_along_axis(
                    row, index, axis=1
                )
        return carry

    for copy in phases:
        copy.wait()
    lax.fori_loop(0, stations, station_table, 0)

    for period in range(periods):
        fetches[period].wait()

        def levels(station, carry):
            for m in range(samples):
                for part in range(2):
                    for half in range(halves):
                        start = lax.div(station, SUB) * (depth * halves * SUB) + half * SUB
                        code = codes[
                            period,
                            m,
                            part,
                            pl.ds(start + lax.rem(station, SUB), depth, stride=halves * SUB),
                            :,
                        ]
                        x_ref[
                            period, m, part, station, :, half * LANES : (half + 1) * LANES
                        ] = (2 * code - 3).astype(f32).astype(bf16)
            return carry

        lax.fori_loop(0, stations, levels, 0)
    for copy in constants:
        copy.wait()
    pl.semaphore_wait(barrier, n_tm - 1 + steps)

    def rows(chunk):
        return pl.ds(chunk * group, group)

    everything = pl.ds(0, count)

    def tm_copy(slot, chunk, block=None):
        block = rows(chunk) if block is None else block
        return pltpu.make_async_remote_copy(
            src_ref=outbox.at[slot - 1, block],
            dst_ref=vis.at[slot, block],
            send_sem=tm_send.at[slot - 1],
            recv_sem=tm_recv.at[slot - 1, chunk],
            device_id={"tm": lax.rem(me + slot, n_tm)},
            device_id_type=MESH,
        )

    def chan_copy(step, chunk, block=None):
        block = rows(chunk) if block is None else block
        return pltpu.make_async_remote_copy(
            src_ref=sends[step].at[block],
            dst_ref=recvs[step].at[block],
            send_sem=ch_send.at[step],
            recv_sem=ch_recv.at[step, chunk],
            device_id={"chan": flip_bits(z, 1 << step)},
            device_id_type=MESH,
        )

    def correlate(slot, chunk):
        base = lax.rem(me + slot, n_tm) * count
        target, index = (vis, 0) if slot == 0 else (outbox, slot - 1)

        def one(k, carry):
            row = chunk * group + k
            a = pairs[0, base + row]
            e = pairs[1, base + row]
            ca, sa = cos_ref[a], sin_ref[a]
            ce, se = cos_ref[e], sin_ref[e]
            cos_diff = ca * ce + sa * se
            sin_diff = sa * ce - ca * se
            for period in range(periods):
                real = imag = None
                for m in range(samples):
                    ar, ai = x_ref[period, m, 0, a], x_ref[period, m, 1, a]
                    er, ei = x_ref[period, m, 0, e], x_ref[period, m, 1, e]
                    step_real = ar * er + ai * ei
                    step_imag = ai * er - ar * ei
                    real = step_real if real is None else real + step_real
                    imag = step_imag if imag is None else imag + step_imag
                real, imag = real.astype(f32), imag.astype(f32)
                both = jnp.concatenate(
                    [real * cos_diff + imag * sin_diff, imag * cos_diff - real * sin_diff], axis=0
                )
                target[index, row, period] = both.astype(bf16)
            return carry

        lax.fori_loop(0, group, one, 0)

    def outgoing(chunk):
        for slot in range(1, n_tm):
            correlate(slot, chunk)
            tm_copy(slot, chunk).start()

    def delay(chunk):
        for slot in range(1, n_tm):
            tm_copy(slot, chunk).wait_recv()

        def one(k, carry):
            row = chunk * group + k
            for slot in range(n_tm):
                for period in range(periods):
                    value = vis[slot, row, period]
                    section = jnp.dot(
                        first_ref[...],
                        jnp.concatenate([value, value], axis=0),
                        preferred_element_type=f32,
                    )
                    yr, yi = section[:outer], section[outer:]
                    tr = yr * tcos_ref[...] + yi * tsin_ref[...]
                    ti = yi * tcos_ref[...] - yr * tsin_ref[...]
                    place = slot * periods + period
                    twisted[place * outer : (place + 1) * outer, :inner] = tr.astype(bf16)
                    twisted[place * outer : (place + 1) * outer, inner:] = ti.astype(bf16)
            parts = []
            sign = jnp.where(
                lax.broadcasted_iota(jnp.int32, (outer, lanes), 1) < lanes // 2, 1.0, -1.0
            )
            for slot in range(n_tm):
                for period in range(periods):
                    place = slot * periods + period
                    both = jnp.dot(
                        twisted[place * outer : (place + 1) * outer],
                        last_ref[...],
                        preferred_element_type=f32,
                    )
                    value = both[:, :lanes] + both[:, lanes:]
                    turned = pltpu.roll(value, lanes // 2, 1) * sign
                    parts.append(((period - periods * slot) % rates, value, turned))
            for rate in range(rates):
                total = None
                for when, value, turned in parts:
                    angle = two_pi * (rate * when % rates) / rates
                    total = add_scaled(total, value, math.cos(angle))
                    total = add_scaled(total, turned, math.sin(angle))
                spec[rate] = total
            for q in range(rates):
                value = spec[flip_bits(z, q)]
                if q % 2 == 0:
                    keep[row, q // 2] = value
                else:
                    sends[0][row, q // 2] = value.astype(bf16)
            return carry

        lax.fori_loop(0, group, one, 0)
        chan_copy(0, chunk).start()

    def combine(step, chunk):
        chan_copy(step, chunk).wait_recv()

        def one(k, carry):
            row = chunk * group + k
            for j in range(recvs[step].shape[1]):
                total = keep[row, j << step] + recvs[step][row, j].astype(f32)
                if step == steps - 1:
                    turned = jnp.transpose(total)
                    half = lanes // 2
                    out_ref[row] = (turned[:half] ** 2 + turned[half:] ** 2) * scale
                elif j % 2 == 0:
                    keep[row, j << step] = total
                else:
                    sends[step + 1][row, j // 2] = total.astype(bf16)
            return carry

        lax.fori_loop(0, group, one, 0)
        if step < steps - 1:
            chan_copy(step + 1, chunk).start()

    for i in range(min(AHEAD, chunks)):
        outgoing(i)

    def round_trip(i, carry):
        @pl.when(i + AHEAD < chunks)
        def _():
            outgoing(i + AHEAD)

        @pl.when(i < chunks)
        def _():
            correlate(0, i)
            delay(i)

        for step in range(steps):
            lag = LAG * (step + 1)

            @pl.when((i >= lag) & (i - lag < chunks))
            def _():
                combine(step, i - lag)

        return carry

    lax.fori_loop(0, chunks + steps * LAG, round_trip, 0)

    for slot in range(1, n_tm):
        tm_copy(slot, 0, everything).wait_send()
    for step in range(steps):
        chan_copy(step, 0, everything).wait_send()


def fringe(n_tm, n_chan, pairs, tones, pcal_phase, samples):
    steps = n_chan.bit_length() - 1
    _, periods, taken, _, stations, width = samples.shape
    depth = width // INNER
    rowed = samples.reshape(periods, taken, 2, stations // SUB, SUB, width // LANES, LANES)
    rowed = rowed.transpose(0, 1, 2, 3, 5, 4, 6).reshape(periods, taken, 2, -1, LANES)
    rates = periods * n_tm
    count = pairs.shape[1] // n_tm
    group = max(g for g in range(1, GROUP + 1) if count % g == 0)
    chunks = count // group
    constants = tables(n_chan, depth)
    firsts, twist_cos, _, last = constants
    outer = twist_cos.shape[0]
    lanes = last.shape[1] // 2
    scale = 1.0 / (100.0 * taken * rates * n_chan * width)
    tile = (outer, lanes)
    boxes = [pltpu.VMEM((count, rates >> (s + 1)) + tile, bf16) for s in range(steps)]
    vmem = pl.BlockSpec(memory_space=pltpu.VMEM)
    stay = pl.BlockSpec(memory_space=pltpu.HBM)
    return pl.pallas_call(
        functools.partial(kernel, n_tm, n_chan, group, scale),
        out_shape=pltpu.VMEM((count, lanes // 2, outer), f32),
        in_specs=[pl.BlockSpec(memory_space=pltpu.SMEM)] + [stay] * 7,
        out_specs=vmem,
        scratch_shapes=[
            pltpu.VMEM((periods, taken, 2, width // LANES * stations, LANES), jnp.int32),
            pltpu.VMEM((periods, taken, 2, stations, depth, INNER), bf16),
            pltpu.VMEM(tones.shape, jnp.int32),
            pltpu.VMEM(pcal_phase.shape[1:], f32),
            pltpu.VMEM((stations, depth, INNER), f32),
            pltpu.VMEM((stations, depth, INNER), f32),
            pltpu.VMEM(firsts.shape[1:], bf16),
            pltpu.VMEM(twist_cos.shape, f32),
            pltpu.VMEM(twist_cos.shape, f32),
            pltpu.VMEM(last.shape, bf16),
            pltpu.VMEM((n_tm, count, periods, 2 * depth, INNER), bf16),
            pltpu.VMEM((n_tm - 1, count, periods, 2 * depth, INNER), bf16),
            pltpu.VMEM((rates * outer, 2 * INNER), bf16),
            pltpu.VMEM((rates,) + tile, f32),
            pltpu.VMEM((count, rates // 2) + tile, f32),
        ]
        + boxes
        + boxes
        + [
            pltpu.SemaphoreType.DMA((2,)),
            pltpu.SemaphoreType.DMA((periods,)),
            pltpu.SemaphoreType.DMA((len(constants),)),
            pltpu.SemaphoreType.DMA((n_tm - 1,)),
            pltpu.SemaphoreType.DMA((n_tm - 1, chunks)),
            pltpu.SemaphoreType.DMA((steps,)),
            pltpu.SemaphoreType.DMA((steps, chunks)),
        ],
        compiler_params=pltpu.CompilerParams(
            collective_id=0, has_side_effects=True, vmem_limit_bytes=57 << 20
        ),
        name="fringe",
    )(pairs, rowed, tones, pcal_phase, *(jnp.asarray(c) for c in constants))


def lending_tables(n_chan, depth, lent):
    firsts, twist_cos, twist_sin, last = tables(n_chan, depth)
    width = 2 * depth
    rows = np.concatenate([np.arange(lent), depth + np.arange(lent)])
    rest = np.concatenate([np.arange(lent, depth), depth + np.arange(lent, depth)])
    own, added = [], []
    for z in range(n_chan):
        high, low = firsts[z][:, :width], firsts[z][:, width:]
        own.append(np.concatenate([high, high, low], axis=1))
        high, low = firsts[z ^ 1][:, :width], firsts[z ^ 1][:, width:]
        added.append(
            np.concatenate(
                [high[:, rows], high[:, rows], low[:, rows], high[:, rest], low[:, rest]], axis=1
            )
        )
    both = np.concatenate([np.stack(own), np.stack(added)], axis=2)
    return both, twist_cos, twist_sin, last


def lending_kernel(n_tm, scale, names, *flat):
    ref = dict(zip(names, flat))
    out_ref, codes, x_ref, lent_x = ref["out"], ref["codes"], ref["x"], ref["lent_x"]
    vis, outbox, lent_vis, lent_box = ref["vis"], ref["outbox"], ref["lent_vis"], ref["lent_box"]
    waves, lent_waves, passed = ref["waves"], ref["lent_waves"], ref["passed"]
    twisted, keep, home_out = ref["twisted"], ref["keep"], ref["home_out"]
    cross_out, sums_in = ref["cross_out"], ref["sums_in"]
    first_ref, tcos_ref, tsin_ref, last_ref = ref["first"], ref["tcos"], ref["tsin"], ref["last"]
    pairs, tones = ref["pairs"], ref["tones"]

    periods, samples, _, stations, depth, inner = x_ref.shape
    lent = lent_x.shape[4]
    count = vis.shape[1]
    pair = 2 if count % 2 == 0 else 1
    rates = periods * n_tm
    outer = tcos_ref.shape[0]
    lanes = last_ref.shape[1] // 2
    halves = inner // LANES
    own_width = 6 * depth
    me = lax.axis_index("tm")
    z = lax.axis_index("chan")
    buddy = flip_bits(z, 1)
    across, far = flip_bits(z, 3), flip_bits(z, 2)
    is_end = lax.rem(z, 3) == 0
    is_inner = lax.rem(z, 3) != 0

    def start_all(copies):
        for copy in copies:
            copy.start()

    def wait_all(copies):
        for copy in copies:
            copy.wait()

    phases = [
        pltpu.make_async_copy(ref["tones_in"], tones, ref["phase_sem"].at[0]),
        pltpu.make_async_copy(ref["pcal_in"].at[0], ref["pcal"], ref["phase_sem"].at[1]),
    ]
    fetches = [
        pltpu.make_async_copy(ref["samples"].at[p], codes.at[p], ref["code_sem"].at[p])
        for p in range(periods)
    ]
    constants = [
        pltpu.make_async_copy(source, target, ref["table_sem"].at[i])
        for i, (source, target) in enumerate(
            [
                (ref["firsts"].at[z], first_ref),
                (ref["tcos_in"], tcos_ref),
                (ref["tsin_in"], tsin_ref),
                (ref["last_in"], last_ref),
            ]
        )
    ]
    start_all(phases + fetches + constants)

    barrier = pltpu.get_barrier_semaphore()
    for slot in range(1, n_tm):
        pl.semaphore_signal(
            barrier, inc=1, device_id={"tm": lax.rem(me + slot, n_tm)}, device_id_type=MESH
        )
    for other in (buddy, far):
        pl.semaphore_signal(barrier, inc=1, device_id={"chan": other}, device_id_type=MESH)

    @pl.when(is_inner)
    def _():
        pl.semaphore_signal(barrier, inc=1, device_id={"chan": across}, device_id_type=MESH)

    def station_tables(source, cos_ref, sin_ref):
        tall = cos_ref.shape[1]

        def one(station, carry):
            phase = ref["pcal"][pl.ds(station, 1), :]
            for turn, target in ((jnp.cos, cos_ref), (jnp.sin, sin_ref)):
                row = jnp.broadcast_to(turn(phase), (tall, LANES))
                for half in range(halves):
                    index = source[pl.ds(half, tall, stride=halves), :]
                    target[station, :, half * LANES : (half + 1) * LANES] = jnp.take_along_axis(
                        row, index, axis=1
                    )
            return carry

        lax.fori_loop(0, stations, one, 0)

    def lend(period):
        return pltpu.make_async_remote_copy(
            src_ref=x_ref.at[period, :, :, :, pl.ds(0, lent)],
            dst_ref=lent_x.at[period],
            send_sem=ref["lend_send"].at[period],
            recv_sem=ref["lend_recv"].at[period],
            device_id={"chan": buddy},
            device_id_type=MESH,
        )

    lend_tones = pltpu.make_async_remote_copy(
        src_ref=tones,
        dst_ref=ref["lent_tones"],
        send_sem=ref["lend_send"].at[periods],
        recv_sem=ref["lend_recv"].at[periods],
        device_id={"chan": buddy},
        device_id_type=MESH,
    )

    wait_all(phases)
    station_tables(tones, ref["cos"], ref["sin"])
    for period in range(periods):
        fetches[period].wait()

        def levels(station, carry):
            for m in range(samples):
                for part in range(2):
                    for half in range(halves):
                        start = lax.div(station, SUB) * (depth * halves * SUB) + half * SUB
                        code = codes[
                            period,
                            m,
                            part,
                            pl.ds(start + lax.rem(station, SUB), depth, stride=halves * SUB),
                            :,
                        ]
                        x_ref[
                            period, m, part, station, :, half * LANES : (half + 1) * LANES
                        ] = (2 * code - 3).astype(f32).astype(bf16)
            return carry

        lax.fori_loop(0, stations, levels, 0)
        if period == 0:

            @pl.when(is_end)
            def _():
                pl.semaphore_wait(barrier, n_tm + 1)
                lend_tones.start()

            @pl.when(is_inner)
            def _():
                pl.semaphore_wait(barrier, n_tm + 2)

        @pl.when(is_end)
        def _():
            lend(period).start()

    wait_all(constants)

    def tm_copy(slot, row, size=1):
        block = pl.ds(row, size)
        return pltpu.make_async_remote_copy(
            src_ref=outbox.at[slot - 1, block],
            dst_ref=vis.at[slot, block],
            send_sem=ref["tm_send"].at[slot - 1],
            recv_sem=ref["tm_recv"].at[slot - 1, lax.div(row, pair)],
            device_id={"tm": lax.rem(me + slot, n_tm)},
            device_id_type=MESH,
        )

    def lent_copy(slot, row, size=1):
        block = pl.ds(row, size)
        return pltpu.make_async_remote_copy(
            src_ref=lent_box.at[slot - 1, block],
            dst_ref=lent_vis.at[slot, block],
            send_sem=ref["tm_lent_send"].at[slot - 1],
            recv_sem=ref["tm_lent_recv"].at[slot - 1, lax.div(row, pair)],
            device_id={"tm": lax.rem(me + slot, n_tm)},
            device_id_type=MESH,
        )

    def pass_copy(row, size=1):
        block = pl.ds(row, size)
        return pltpu.make_async_remote_copy(
            src_ref=passed.at[block],
            dst_ref=passed.at[block],
            send_sem=ref["pass_send"],
            recv_sem=ref["pass_recv"].at[row],
            device_id={"chan": buddy},
            device_id_type=MESH,
        )

    def sum_copy(index, row):
        block = pl.ds(row, 1)
        return pltpu.make_async_remote_copy(
            src_ref=cross_out.at[index, block],
            dst_ref=sums_in.at[0, block],
            send_sem=ref["cross_send"],
            recv_sem=ref["sum_recv"].at[row],
            device_id={"chan": far if index else across},
            device_id_type=MESH,
        )

    def home_copy(row, size=1):
        block = pl.ds(row, size)
        return pltpu.make_async_remote_copy(
            src_ref=home_out.at[block],
            dst_ref=sums_in.at[1, block],
            send_sem=ref["home_send"],
            recv_sem=ref["pass_recv"].at[row],
            device_id={"chan": buddy},
            device_id_type=MESH,
        )

    cross_drain = pltpu.make_async_copy(cross_out, cross_out, ref["cross_send"])

    def correlate(slot, row, voltage, cos_ref, sin_ref, target, index):
        place = lax.rem(me + slot, n_tm) * count + row
        a = pairs[0, place]
        e = pairs[1, place]
        ca, sa = cos_ref[a], sin_ref[a]
        ce, se = cos_ref[e], sin_ref[e]
        cos_diff = ca * ce + sa * se
        sin_diff = sa * ce - ca * se
        for period in range(periods):
            real = imag = None
            for m in range(samples):
                ar, ai = voltage[period, m, 0, a], voltage[period, m, 1, a]
                er, ei = voltage[period, m, 0, e], voltage[period, m, 1, e]
                step_real = ar * er + ai * ei
                step_imag = ai * er - ar * ei
                real = step_real if real is None else real + step_real
                imag = step_imag if imag is None else imag + step_imag
            real, imag = real.astype(f32), imag.astype(f32)
            both = jnp.concatenate(
                [real * cos_diff + imag * sin_diff, imag * cos_diff - real * sin_diff], axis=0
            )
            target[index, row, period] = both.astype(bf16)

    def own_visibility(slot, row):
        target, index = (vis, 0) if slot == 0 else (outbox, slot - 1)
        correlate(slot, row, x_ref, ref["cos"], ref["sin"], target, index)

    def lent_visibility(slot, row):
        target, index = (lent_vis, 0) if slot == 0 else (lent_box, slot - 1)
        correlate(slot, row, lent_x, ref["lent_cos"], ref["lent_sin"], target, index)

    def outgoing(row):
        for slot in range(1, n_tm):
            own_visibility(slot, row)

            @pl.when(lax.rem(row, pair) == pair - 1)
            def _():
                tm_copy(slot, row - (pair - 1), pair).start()

    def lent_outgoing(row):
        for slot in range(1, n_tm):
            lent_visibility(slot, row)

            @pl.when(lax.rem(row, pair) == pair - 1)
            def _():
                lent_copy(slot, row - (pair - 1), pair).start()

    def spectra(source, row, target):
        tall = target.shape[1] // 2
        parts = []
        for slot in range(n_tm):
            for period in range(periods):
                value = source[slot, row, period].astype(f32)
                parts.append(((period - periods * slot) % rates, value[:tall], value[tall:]))
        for rate in range(rates):
            real = imag = None
            for when, vr, vi in parts:
                angle = two_pi * (rate * when % rates) / rates
                c, s = math.cos(angle), math.sin(angle)
                real = add_scaled(add_scaled(real, vr, c), vi, s)
                imag = add_scaled(add_scaled(imag, vi, c), vr, -s)
            target[rate, :tall] = real
            target[rate, tall:] = imag

    def halves_of(value):
        high = value.astype(bf16)
        low = (value - high.astype(f32)).astype(bf16)
        return [high, low, high]

    def stage_one(place, columns, blocks):
        section = jnp.dot(
            columns, jnp.concatenate(blocks, axis=0), preferred_element_type=f32
        )
        yr, yi = section[:outer], section[outer:]
        tr = yr * tcos_ref[...] + yi * tsin_ref[...]
        ti = yi * tcos_ref[...] - yr * tsin_ref[...]
        twisted[place * outer : (place + 1) * outer, :inner] = tr.astype(bf16)
        twisted[place * outer : (place + 1) * outer, inner:] = ti.astype(bf16)

    def stage_two(place):
        both = jnp.dot(
            twisted[place * outer : (place + 1) * outer],
            last_ref[...],
            preferred_element_type=f32,
        )
        return both[:, :lanes] + both[:, lanes:]

    def finish(row, total):
        turned = jnp.transpose(total)
        half = lanes // 2
        out_ref[row] = (turned[:half] ** 2 + turned[half:] ** 2) * scale

    @pl.when(is_end)
    def _():
        def send_rows(row, carry):
            outgoing(row)
            return carry

        lax.fori_loop(0, count, send_rows, 0)

        def one(row, carry):
            own_visibility(0, row)

            @pl.when(lax.rem(row, pair) == 0)
            def _():
                for slot in range(1, n_tm):
                    tm_copy(slot, row, pair).wait_recv()

            spectra(vis, row, waves)
            for q in range(1, rates):
                value = waves[flip_bits(z, q)]
                rest = jnp.concatenate([value[lent:depth], value[depth + lent :]], axis=0)
                passed[row, q - 1] = rest.astype(bf16)
            pass_copy(row).start()
            stage_one(0, first_ref[:, :own_width], halves_of(waves[z]))
            keep[row] = stage_two(0)
            return carry

        lax.fori_loop(0, min(EARLY, count), one, 0)
        lend_tones.wait_send()
        for period in range(periods):
            lend(period).wait_send()
        lax.fori_loop(min(EARLY, count), count, one, 0)

        def close(row, carry):
            home_copy(row).wait_recv()
            sum_copy(1, row).wait_recv()
            finish(row, keep[row] + sums_in[0, row].astype(f32) + sums_in[1, row].astype(f32))
            return carry

        lax.fori_loop(0, count, close, 0)
        pass_copy(0, count).wait_send()

    @pl.when(is_inner)
    def _():
        def send_rows(row, carry):
            outgoing(row)
            return carry

        lax.fori_loop(0, min(FAR_AHEAD, count), send_rows, 0)
        lend_tones.wait_recv()
        station_tables(ref["lent_tones"], ref["lent_cos"], ref["lent_sin"])
        for period in range(periods):
            lend(period).wait_recv()

        def lend_rows(row, carry):
            lent_outgoing(row)
            return carry

        lax.fori_loop(0, min(LENT_AHEAD, count), lend_rows, 0)

        def one(row, carry):
            @pl.when(row + FAR_AHEAD < count)
            def _():
                outgoing(row + FAR_AHEAD)

            @pl.when(row + LENT_AHEAD < count)
            def _():
                lent_outgoing(row + LENT_AHEAD)

            @pl.when(row < count)
            def _():
                own_visibility(0, row)
                lent_visibility(0, row)

                @pl.when(lax.rem(row, pair) == 0)
                def _():
                    for slot in range(1, n_tm):
                        tm_copy(slot, row, pair).wait_recv()

                spectra(vis, row, waves)

                @pl.when(lax.rem(row, pair) == 0)
                def _():
                    for slot in range(1, n_tm):
                        lent_copy(slot, row, pair).wait_recv()

                spectra(lent_vis, row, lent_waves)
                stage_one(1, first_ref[:, :own_width], halves_of(waves[buddy]))
                pass_copy(row).wait_recv()
                for q in range(rates):
                    if q != 1:
                        rate = flip_bits(z, q)
                        arrived = passed[row, (q ^ 1) - 1]
                        blocks = halves_of(waves[rate]) + halves_of(lent_waves[rate])
                        stage_one(q, first_ref[...], blocks + [arrived, arrived])
                keep[row] = stage_two(0)
                home_out[row] = stage_two(1).astype(bf16)
                cross_out[1, row] = stage_two(2).astype(bf16)
                cross_out[0, row] = stage_two(3).astype(bf16)
                sum_copy(1, row).start()
                sum_copy(0, row).start()
                home_copy(row).start()

            @pl.when(row >= LAG)
            def _():
                late = row - LAG
                sum_copy(0, late).wait_recv()
                finish(late, keep[late] + sums_in[0, late].astype(f32))

            return carry

        lax.fori_loop(0, count + LAG, one, 0)
        for slot in range(1, n_tm):
            lent_copy(slot, jnp.int32(0), count).wait_send()
        cross_drain.wait()
        home_copy(0, count).wait_send()

    for slot in range(1, n_tm):
        tm_copy(slot, jnp.int32(0), count).wait_send()


def fringe_lending(n_tm, n_chan, pairs, tones, pcal_phase, samples):
    _, periods, taken, _, stations, width = samples.shape
    depth = width // INNER
    lent = min(LENT, depth // 2)
    rowed = samples.reshape(periods, taken, 2, stations // SUB, SUB, width // LANES, LANES)
    rowed = rowed.transpose(0, 1, 2, 3, 5, 4, 6).reshape(periods, taken, 2, -1, LANES)
    rates = periods * n_tm
    count = pairs.shape[1] // n_tm
    constants = lending_tables(n_chan, depth, lent)
    firsts, twist_cos, _, last = constants
    outer = twist_cos.shape[0]
    lanes = last.shape[1] // 2
    scale = 1.0 / (100.0 * taken * rates * n_chan * width)
    tile = (outer, lanes)
    dma = pltpu.SemaphoreType.DMA
    pairs_of = count // 2 if count % 2 == 0 else count
    kept = {
        "codes": pltpu.VMEM((periods, taken, 2, width // LANES * stations, LANES), jnp.int32),
        "x": pltpu.VMEM((periods, taken, 2, stations, depth, INNER), bf16),
        "lent_x": pltpu.VMEM((periods, taken, 2, stations, lent, INNER), bf16),
        "tones": pltpu.VMEM(tones.shape, jnp.int32),
        "lent_tones": pltpu.VMEM(tones.shape, jnp.int32),
        "pcal": pltpu.VMEM(pcal_phase.shape[1:], f32),
        "cos": pltpu.VMEM((stations, depth, INNER), f32),
        "sin": pltpu.VMEM((stations, depth, INNER), f32),
        "lent_cos": pltpu.VMEM((stations, lent, INNER), f32),
        "lent_sin": pltpu.VMEM((stations, lent, INNER), f32),
        "first": pltpu.VMEM(firsts.shape[1:], bf16),
        "tcos": pltpu.VMEM(twist_cos.shape, f32),
        "tsin": pltpu.VMEM(twist_cos.shape, f32),
        "last": pltpu.VMEM(last.shape, bf16),
        "vis": pltpu.VMEM((n_tm, count, periods, 2 * depth, INNER), bf16),
        "outbox": pltpu.VMEM((n_tm - 1, count, periods, 2 * depth, INNER), bf16),
        "lent_vis": pltpu.VMEM((n_tm, count, periods, 2 * lent, INNER), bf16),
        "lent_box": pltpu.VMEM((n_tm - 1, count, periods, 2 * lent, INNER), bf16),
        "waves": pltpu.VMEM((rates, 2 * depth, INNER), f32),
        "lent_waves": pltpu.VMEM((rates, 2 * lent, INNER), f32),
        "passed": pltpu.VMEM((count, rates - 1, 2 * (depth - lent), INNER), bf16),
        "twisted": pltpu.VMEM((rates * outer, 2 * INNER), bf16),
        "keep": pltpu.VMEM((count,) + tile, f32),
        "home_out": pltpu.VMEM((count,) + tile, bf16),
        "cross_out": pltpu.VMEM((2, count) + tile, bf16),
        "sums_in": pltpu.VMEM((2, count) + tile, bf16),
        "phase_sem": dma((2,)),
        "code_sem": dma((periods,)),
        "table_sem": dma((len(constants),)),
        "lend_send": dma((periods + 1,)),
        "lend_recv": dma((periods + 1,)),
        "tm_send": dma((n_tm - 1,)),
        "tm_recv": dma((n_tm - 1, pairs_of)),
        "tm_lent_send": dma((n_tm - 1,)),
        "tm_lent_recv": dma((n_tm - 1, pairs_of)),
        "pass_send": dma,
        "pass_recv": dma((count,)),
        "cross_send": dma,
        "home_send": dma,
        "sum_recv": dma((count,)),
    }
    given = ["pairs", "samples", "tones_in", "pcal_in", "firsts", "tcos_in", "tsin_in", "last_in"]
    vmem = pl.BlockSpec(memory_space=pltpu.VMEM)
    stay = pl.BlockSpec(memory_space=pltpu.HBM)
    return pl.pallas_call(
        functools.partial(lending_kernel, n_tm, scale, given + ["out"] + list(kept)),
        out_shape=pltpu.VMEM((count, lanes // 2, outer), f32),
        in_specs=[pl.BlockSpec(memory_space=pltpu.SMEM)] + [stay] * 7,
        out_specs=vmem,
        scratch_shapes=list(kept.values()),
        compiler_params=pltpu.CompilerParams(
            collective_id=0, has_side_effects=True, vmem_limit_bytes=57 << 20
        ),
        name="fringe_lending",
    )(pairs, rowed, tones, pcal_phase, *(jnp.asarray(c) for c in constants))


def shards(samples, pcal_phase, tone_index, baseline_pairs):
    n_chan = lax.axis_size("chan")
    search = fringe_lending if n_chan == 4 else fringe
    power = search(
        lax.axis_size("tm"),
        n_chan,
        baseline_pairs.T,
        tone_index.reshape(-1, LANES),
        pcal_phase,
        samples,
    )
    return power.reshape(1, 1, power.shape[0], ND)


def solution(mesh):
    placed = (
        P("pol", ("scan", "tm"), None, None, None, "chan"),
        P("pol", None, None),
        P("chan"),
        P(),
    )
    return jax.shard_map(
        shards,
        mesh=mesh,
        in_specs=placed,
        out_specs=P("pol", ("scan", "chan"), "tm", None),
        check_vma=False,
    )
```
